32 devices in a mesh: section: 2 (over x), dp: 16 (over z, y, core).
Axes of the slice: x: 2, y: 2, z: 4, core: 2. Of those that a mesh axis runs over, the one named last changes fastest.
Arguments:
- activations: bfloat16 [2, 8, 768, 5376], P('section', None, 'dp'), may hold values from -6 to 6
- loss_grads: bfloat16 [8, 768, 5376], P(None, 'dp'), may hold values from -6 to 6
- adapter_in: bfloat16 [2, 5376, 64], P('section'), may hold values from -0.078125 to 0.078125
- adapter_out: bfloat16 [2, 64, 5376], P('section'), may hold values from -0.75 to 0.75
- first_moment: float32 [2, 16, 86016], P('section', 'dp'), may hold values from -0.4 to 0.4
- second_moment: float32 [2, 16, 86016], P('section', 'dp'), may hold values from 0.0001 to 0.01
- old_owner: int32 [2, 8], P('section'), may hold values from 0 to 15, as said below
- new_owner: int32 [2, 16], P('section'), may hold values from 0 to 15, each once within a row
- plan: int32 [8], replicated, may hold values from 0 to 7, each once
Outputs:
- input_grads: bfloat16 [2, 8, 768, 5376], P('section', None, 'dp')
- adam_update: float32 [2, 16, 43008], P('section', 'dp')
- first_new: float32 [2, 16, 43008], P('section', 'dp')
- second_new: float32 [2, 16, 43008], P('section', 'dp')
The draws below stay inside these ranges and needn't reach their ends.
Inputs may be any that keep to these rules, and one draw needn't show every extreme that they name: `old_owner`: the entries of one section's row are distinct.
All inputs are finite; a program needn't handle non-finite values.
Results may differ from the reference program's by a relative error of at most 0.025.
Values may be sent and summed in bfloat16 or wider, within the bound.
A program may use at most 64 MiB of HBM per device.

```python
import math
import jax
import jax.numpy as jnp

D = 5376
RANK = 64
MB = 8
SECTIONS = 2
TOKENS = 768
BLOCK = 43008
OLD_DP = 8
N_DP = 16


def draw_old_owner(key, part):
    section_keys = jax.random.split(key, SECTIONS)
    rows = jax.vmap(lambda section_key: jax.random.permutation(section_key, N_DP)[:OLD_DP])(section_keys)
    return rows.astype(jnp.int32)


def strengthened(drawn, key, source, target, parts, factor):
    owner, partner = [(jnp.arange(drawn.shape[axis_at]) // (drawn.shape[axis_at] // parts)).reshape([-1 if axis == axis_at else 1 for axis in range(drawn.ndim)]) for axis_at in (source, target)]
    chosen = jax.random.permutation(key, parts)[partner]
    strong = (owner == chosen) | (owner == (partner + parts // 2) % parts)
    return jnp.where(strong, factor * drawn, drawn)


def levels(key, shape, cuts, low, largest):
    loudness, own = 1.0, jax.random.fold_in(key, 6)
    for dim, blocks in cuts:
        steps = jnp.exp(jax.random.uniform(jax.random.fold_in(own, dim), (blocks,), jnp.float32, low / len(cuts), largest / len(cuts)))
        loudness = loudness * jnp.repeat(steps, shape[dim] // blocks).reshape([-1 if axis == dim else 1 for axis in range(len(shape))])
    return loudness


def bell_draw(stream_key, shape, width, bound, cuts=(), kind=jnp.bfloat16):
    array = jax.random.normal(stream_key, shape, jnp.float32) * width
    if len(cuts) > 0:
        array = levels(stream_key, shape, cuts, -0.22, 0.18) * array
    return jnp.clip(array, min=-bound, max=bound).astype(kind)


def heavy_noise(rng, dims, width, reach, shards, heavy, kind=jnp.bfloat16):
    array = width * jax.random.normal(rng, dims, jnp.float32)
    if shards:
        array = array * levels(rng, dims, shards, -0.22, 0.18)
    return jnp.clip(strengthened(array, jax.random.fold_in(rng, 3), *heavy), -reach, reach).astype(kind)


def setup_inputs(seed: int = 0) -> dict:
    key_of = jax.random.split(jax.random.key(seed), 10)
    activations = bell_draw(key_of[0], (SECTIONS, MB, TOKENS, D), 1.0, 6.0, ((0, 2), (2, 16)))
    loss_grads = heavy_noise(key_of[1], (MB, TOKENS, D), 1.0, 6.0, ((1, 16),), (1, 2, 16, 2.0))
    adapter_in = bell_draw(key_of[2], (SECTIONS, D, RANK), D ** -0.5, 0.078125, ((0, 2),))
    adapter_out = bell_draw(key_of[3], (SECTIONS, RANK, D), RANK ** -0.5, 0.75, ((0, 2),))
    first_moment = bell_draw(key_of[4], (SECTIONS, N_DP, 2 * BLOCK), 0.05, 0.4, ((0, 2), (1, 16)), jnp.float32)
    second_moment = jnp.clip(jnp.exp(math.log(0.01) - 4.6051702 * jax.random.uniform(key_of[5], (SECTIONS, N_DP, 2 * BLOCK), jnp.float32) ** levels(key_of[5], (SECTIONS, N_DP, 2 * BLOCK), ((0, 2), (1, 16)), -0.2, 0.2)), 0.0001, 0.01)
    old_owner = draw_old_owner(jax.random.fold_in(key_of[9], 71), 0)
    new_owner = jax.vmap(lambda own: jax.random.permutation(own, N_DP))(jax.random.split(key_of[7], SECTIONS)).reshape((SECTIONS, N_DP)).astype(jnp.int32)
    plan = jax.random.permutation(key_of[8], MB).astype(jnp.int32)
    return dict(activations=activations, loss_grads=loss_grads, adapter_in=adapter_in, adapter_out=adapter_out, first_moment=first_moment, second_moment=second_moment, old_owner=old_owner, new_owner=new_owner, plan=plan)


beta_one = 0.9
beta_two = 0.95
adam_eps = 1e-08
adam_step = 1000.0
loss_scale = 4096.0

def silu_slope(pre_value):
    gate_value = jax.nn.sigmoid(pre_value)
    return gate_value * (1.0 + pre_value * (1.0 - gate_value))

def adam_rows(grads, first, second):
    first_next = beta_one * first + (1.0 - beta_one) * grads
    second_next = beta_two * second + (1.0 - beta_two) * grads * grads
    update = first_next / (1.0 - beta_one ** adam_step) / (jnp.sqrt(second_next / (1.0 - beta_two ** adam_step)) + adam_eps)
    return (update, first_next, second_next)

def reference(activations, loss_grads, adapter_in, adapter_out, first_moment, second_moment, old_owner, new_owner, plan):
    incoming = loss_grads[plan]
    emitted = []
    updates = []
    firsts = []
    seconds = []
    for section_index in reversed(range(SECTIONS)):
        section_input = activations[section_index][plan].reshape(-1, D)
        incoming_flat = incoming.reshape(-1, D)
        weight_in = adapter_in[section_index]
        weight_out = adapter_out[section_index]
        pre_value = jnp.dot(section_input, weight_in, preferred_element_type=jnp.float32)
        hidden = jax.nn.silu(pre_value).astype(jnp.bfloat16)
        act_grad = jnp.dot(incoming_flat, weight_out.T, preferred_element_type=jnp.float32)
        pre_grad = (act_grad * silu_slope(pre_value)).astype(jnp.bfloat16)
        input_grad = (incoming_flat.astype(jnp.float32) + jnp.dot(pre_grad, weight_in.T, preferred_element_type=jnp.float32)).astype(jnp.bfloat16)
        grad_in = jnp.dot(section_input.T, pre_grad, preferred_element_type=jnp.float32)
        grad_out = jnp.dot(hidden.T, incoming_flat, preferred_element_type=jnp.float32)
        grads = jnp.concatenate([grad_in.reshape(-1), grad_out.reshape(-1)]) / loss_scale
        first_old = first_moment[section_index][old_owner[section_index]].reshape(-1)
        second_old = second_moment[section_index][old_owner[section_index]].reshape(-1)
        update, first_next, second_next = adam_rows(grads, first_old, second_old)
        inverse = jnp.argsort(new_owner[section_index]).astype(jnp.int32)
        updates.insert(0, update.reshape(N_DP, BLOCK)[inverse])
        firsts.insert(0, first_next.reshape(N_DP, BLOCK)[inverse])
        seconds.insert(0, second_next.reshape(N_DP, BLOCK)[inverse])
        incoming = input_grad.reshape(MB, TOKENS, D)
        emitted.insert(0, incoming)
    return (jnp.stack(emitted), jnp.stack(updates), jnp.stack(firsts), jnp.stack(seconds))
```

```python
import functools
import math

import jax
import jax.numpy as jnp
from jax import lax
from jax.experimental import pallas as pl
from jax.experimental.pallas import tpu as pltpu
from jax.sharding import PartitionSpec as P

beta_one = 0.9
beta_two = 0.95
adam_eps = 1e-08
adam_step = 1000.0
loss_scale = 4096.0
MESH = pl.DeviceIdType.MESH
VMEM = pl.BlockSpec(memory_space=pltpu.VMEM)
SMEM = pl.BlockSpec(memory_space=pltpu.SMEM)
ANY = pl.BlockSpec(memory_space=pl.ANY)
HBM = pl.BlockSpec(memory_space=pltpu.HBM)


def nt_dot(left, right):
    return lax.dot_general(left, right, (((1,), (1,)), ((), ())), preferred_element_type=jnp.float32)


def column_width(width):
    return 128 * max(d for d in range(1, 8) if (width // 128) % d == 0)


def greet(n, me, extra):
    barrier = pltpu.get_barrier_semaphore()

    @pl.loop(1, n)
    def _(d):
        pl.semaphore_signal(barrier, inc=1, device_id={"dp": lax.rem(me + d, n)}, device_id_type=MESH)

    if extra is not None:
        pl.semaphore_signal(barrier, inc=1, device_id={"section": extra}, device_id_type=MESH)
    pl.semaphore_wait(barrier, n - 1 + (extra is not None))


def relay_kernel(
    n, block_rows, pad,
    new_hbm, old_hbm, plan_hbm, x_hbm, l_hbm, win_hbm, wout_hbm, m_hbm, v_hbm,
    o_ref, total_ref, first_ref, second_ref,
    new_ref, old_ref, plan_ref, order, x_buf, l_buf, win_buf, wout_buf, m_buf, v_buf, w_ref, mix,
    p_buf, p_up, p_now, pieces, spread, chosen, got, gin, gout, turn, acc,
    blocks, outbox, near, summed, mid, far,
    i_sem, g_sem, x_sem, l_sem, w_send, w_recv, f_send, f_recv, k_send, k_recv, p_send, p_recv,
    a_send, a_recv, b_send, b_recv, own_sem, s1, r1, s2, r2, s3, r3,
):
    me = lax.axis_index("dp")
    section = lax.axis_index("section")
    other = 1 - section
    core = lax.rem(me, 2)
    sibling = me + 1 - 2 * core
    chip = me // 2
    chips = n // 2
    pairs = chips // 2
    lane = lax.rem(chip, 2)
    pair = chip // 2
    across = (pair * 2 + 1 - lane) * 2
    rank, width = win_hbm.shape
    cw = column_width(width)
    chunks = width // cw
    tiles = width // 128
    lines = block_rows // tiles

    barrier = pltpu.get_barrier_semaphore()

    @pl.loop(1, n)
    def _(d):
        pl.semaphore_signal(barrier, inc=1, device_id={"dp": lax.rem(me + d, n)}, device_id_type=MESH)

    pl.semaphore_signal(barrier, inc=1, device_id={"section": other}, device_id_type=MESH)

    def started(src, dst, sem):
        load = pltpu.make_async_copy(src, dst, sem)
        load.start()
        return load

    ints = [
        started(src, dst, i_sem.at[k])
        for k, (src, dst) in enumerate(((new_hbm, new_ref), (old_hbm, old_ref), (plan_hbm, plan_ref)))
    ]
    weights = [
        started(src, dst, g_sem.at[k])
        for k, (src, dst) in enumerate(
            ((win_hbm, win_buf), (m_hbm, m_buf), (v_hbm, v_buf), (wout_hbm, wout_buf))
        )
    ]
    loads = []
    for c in range(chunks):
        cols = pl.ds(c * cw, cw)
        loads.append(started(x_hbm.at[:, :, cols], x_buf.at[:, :, cols], x_sem.at[c]))
        loads.append(started(l_hbm.at[:, :, cols], l_buf.at[:, :, cols], l_sem.at[c]))

    half, quarter = rank // 2, rank // 4

    def rows_of(core_at, lane_at):
        return pl.ds(pl.multiple_of(core_at * half + lane_at * quarter, quarter), quarter)

    parts = (rows_of(core, lane), rows_of(core, 1 - lane))
    their_parts = (rows_of(1 - core, lane), rows_of(1 - core, 1 - lane))

    def w_copy(k):
        return pltpu.make_async_remote_copy(
            win_buf.at[parts[k]], w_ref.at[parts[k]], w_send.at[k], w_recv.at[k],
            device_id={"section": other}, device_id_type=MESH,
        )

    def forward(k):
        return pltpu.make_async_remote_copy(
            w_ref.at[parts[k]], w_ref.at[parts[k]], f_send.at[k], f_recv.at[k],
            device_id={"dp": sibling}, device_id_type=MESH,
        )

    def forwarded(k):
        return pltpu.make_async_remote_copy(
            w_ref.at[their_parts[k]], w_ref.at[their_parts[k]], f_send.at[k], f_recv.at[k],
            device_id={"dp": sibling}, device_id_type=MESH,
        )

    mix_peers = (
        (sibling, rows_of(1 - core, lane)),
        (across + core, rows_of(core, 1 - lane)),
        (across + 1 - core, rows_of(1 - core, 1 - lane)),
    )

    def mix_copy(k):
        return pltpu.make_async_remote_copy(
            mix.at[parts[0]], mix.at[parts[0]], k_send.at[k], k_recv.at[k],
            device_id={"dp": mix_peers[k][0]}, device_id_type=MESH,
        )

    def mix_arrival(k):
        rows = mix_peers[k][1]
        return pltpu.make_async_remote_copy(
            mix.at[rows], mix.at[rows], k_send.at[k], k_recv.at[k],
            device_id={"dp": mix_peers[k][0]}, device_id_type=MESH,
        )

    p_copy = pltpu.make_async_remote_copy(
        p_buf, p_up, p_send, p_recv, device_id={"section": other}, device_id_type=MESH
    )

    def spread_copy(d):
        peer = lax.rem(me + d, n)
        return pltpu.make_async_remote_copy(
            pieces.at[peer], spread.at[me], a_send.at[d], a_recv.at[d],
            device_id={"dp": peer}, device_id_type=MESH,
        )

    def spread_arrival(d):
        peer = lax.rem(me + n - d, n)
        return pltpu.make_async_remote_copy(
            pieces.at[peer], spread.at[peer], a_send.at[d], a_recv.at[d],
            device_id={"dp": peer}, device_id_type=MESH,
        )

    def gather_copy(d):
        peer = lax.rem(me + d, n)
        return pltpu.make_async_remote_copy(
            chosen.at[peer], got.at[me], b_send.at[d], b_recv.at[d],
            device_id={"dp": peer}, device_id_type=MESH,
        )

    def gather_arrival(d):
        peer = lax.rem(me + n - d, n)
        return pltpu.make_async_remote_copy(
            chosen.at[peer], got.at[peer], b_send.at[d], b_recv.at[d],
            device_id={"dp": peer}, device_id_type=MESH,
        )

    def near_copy(to):
        return pltpu.make_async_remote_copy(
            outbox.at[to], near.at[to], s1.at[to], r1.at[to], device_id={"dp": sibling}, device_id_type=MESH
        )

    def mid_copy(at):
        return pltpu.make_async_remote_copy(
            summed.at[at * 2 + 1 - lane], mid.at[at], s3.at[at], r3.at[at],
            device_id={"dp": across + core}, device_id_type=MESH,
        )

    def far_copy(d):
        to = lax.rem(pair + d, pairs) * 2 + lane
        return pltpu.make_async_remote_copy(
            summed.at[to], far.at[d], s2.at[d], r2.at[d],
            device_id={"dp": to * 2 + core}, device_id_type=MESH,
        )

    weights[0].wait()
    pl.semaphore_wait(barrier, n)
    w_copy(0).start()

    part = block_rows // n
    slab = pieces.shape[2] // 2
    filler = [jnp.zeros((slab - part, 128), jnp.float32)] if slab > part else []
    weights[1].wait()
    weights[2].wait()
    for t in range(n):
        for h in range(2):
            start = h * block_rows + t * part
            pieces[t, h] = jnp.concatenate(
                [m_buf[start : start + part, :]] + filler + [v_buf[start : start + part, :]] + filler, axis=0
            ).astype(jnp.bfloat16)

    @pl.loop(1, n)
    def _(d):
        spread_copy(d).start()

    own = started(pieces.at[me], spread.at[me], own_sem.at[0])
    for load in ints:
        load.wait()
    owners = [new_ref[c] for c in range(n)]
    for t in range(n):
        block = jnp.int32(0)
        for c in range(1, n):
            block = jnp.where(owners[c] == t, c, block)
        order[t] = block
    for b in range(chips):
        blocks[b, block_rows:, :] = jnp.zeros((pad, 128), jnp.bfloat16)

    micro_count, tok_rows, _ = x_buf.shape
    rows = micro_count * tok_rows

    def tokens(ref, cols):
        return ref[:, :, cols].reshape(rows, -1)

    pre = jnp.zeros((rows, rank), jnp.float32)
    act = jnp.zeros((rows, rank), jnp.float32)
    weights[3].wait()
    for c in range(chunks):
        cols = pl.ds(c * cw, cw)
        loads[2 * c].wait()
        pre = pre + nt_dot(tokens(x_buf, cols), win_buf[:, cols])
        loads[2 * c + 1].wait()
        act = act + nt_dot(tokens(l_buf, cols), wout_buf[:, cols])
    slope = silu_slope(pre)
    p_buf[...] = (act * slope).astype(jnp.bfloat16).reshape(p_buf.shape)
    p_copy.start()
    w_copy(1).start()
    hidden_t = jax.nn.silu(pre).T.astype(jnp.bfloat16)

    w_copy(0).wait_recv()
    forward(0).start()
    mixed = nt_dot(w_ref[parts[0], :], wout_buf[...])
    mix[parts[0], :] = jnp.concatenate([mixed, jnp.zeros((quarter, 128 - rank), jnp.float32)], axis=1).astype(
        jnp.bfloat16
    )
    for k in range(3):
        mix_copy(k).start()

    for c in range(chunks):
        cols = pl.ds(c * cw, cw)
        gout[:, cols] = jnp.dot(hidden_t, tokens(l_buf, cols), preferred_element_type=jnp.float32)
    for b in range(chips):
        for t in range(tiles):
            turn[pl.ds(t, lines, stride=tiles), :] = gout[b * lines : (b + 1) * lines, t * 128 : (t + 1) * 128]
        blocks[chips + b, :block_rows, :] = turn[...].astype(jnp.bfloat16)

    p_copy.wait_recv()
    p_in = jnp.where(section == 0, p_up[...].astype(jnp.float32), 0.0).astype(jnp.bfloat16)
    p_up[...] = p_in
    p_in = p_in.reshape(rows, rank)
    shared = jnp.dot(hidden_t, p_in, preferred_element_type=jnp.float32)
    shared = jnp.concatenate([shared, jnp.zeros((rank, 128 - rank), jnp.float32)], axis=1)
    for b in range(chips):
        blocks[chips + b, block_rows:, :] = jnp.concatenate(
            [shared[b * lines : (b + 1) * lines, :], jnp.zeros((pad - lines, 128), jnp.float32)], axis=0
        ).astype(jnp.bfloat16)
    for k in range(3):
        mix_arrival(k).wait_recv()
    grad = (act + jnp.dot(p_in, mix[:, :rank], preferred_element_type=jnp.float32)) * slope
    p_now[...] = grad.astype(jnp.bfloat16).reshape(p_now.shape)
    p_t = grad.T.astype(jnp.bfloat16)
    for c in range(chunks):
        cols = pl.ds(c * cw, cw)
        gin[cols, :] = jnp.dot(p_t, tokens(x_buf, cols), preferred_element_type=jnp.float32).T
    for b in range(chips):
        start = b * block_rows * 2
        low = gin[pl.ds(start, block_rows, stride=2), :]
        high = gin[pl.ds(start + 1, block_rows, stride=2), :]
        blocks[b, :block_rows, :] = jnp.concatenate([low, high], axis=1).astype(jnp.bfloat16)

    for side in (1 - lane, lane):

        @pl.loop(0, pairs)
        def _(at):
            to = at * 2 + side
            outbox[to] = blocks[order[to * 2 + 1 - core]]
            near_copy(to).start()

    @pl.loop(0, pairs)
    def _(at):
        to = at * 2 + 1 - lane
        near_copy(to).wait_recv()
        summed[to] = (
            blocks[order[to * 2 + core]].astype(jnp.float32) + near[to].astype(jnp.float32)
        ).astype(jnp.bfloat16)
        mid_copy(at).start()

    own.wait()

    @pl.loop(1, n)
    def _(d):
        spread_arrival(d).wait_recv()

    for t in range(n):
        block = order[t]
        chosen[t] = spread[old_ref[block // 2], lax.rem(block, 2)]

    @pl.loop(1, n)
    def _(d):
        gather_copy(d).start()

    keep = started(chosen.at[me], got.at[me], own_sem.at[1])
    w_copy(1).wait_recv()
    forward(1).start()


    def drained(ref, cols):
        return jnp.concatenate([ref[plan_ref[m], :, cols] for m in range(micro_count)], axis=0)

    p_up_turn, p_now_turn = drained(p_up, slice(None)), drained(p_now, slice(None))
    forwarded(0).wait_recv()
    forwarded(1).wait_recv()

    def emit(c):
        cols = pl.ds(c * cw, cw)
        incoming = (
            drained(l_buf, cols).astype(jnp.float32) + jnp.dot(p_up_turn, w_ref[:, cols], preferred_element_type=jnp.float32)
        ).astype(jnp.bfloat16)
        o_ref[:, cols] = (
            incoming.astype(jnp.float32)
            + jnp.dot(p_now_turn, win_buf[:, cols], preferred_element_type=jnp.float32)
        ).astype(jnp.bfloat16)

    emitted = 0
    for at in range(pairs):
        until = -(-chunks * (at + 1) // pairs)
        for c in range(emitted, until):
            emit(c)
        emitted = until
        to = at * 2 + lane
        near_copy(to).wait_recv()
        mid_copy(at).wait_recv()
        joined = (
            blocks[order[to * 2 + core]].astype(jnp.float32)
            + near[to].astype(jnp.float32)
            + mid[at].astype(jnp.float32)
        )

        @pl.when(pair != at)
        def _():
            summed[to] = joined.astype(jnp.bfloat16)
            far_copy(lax.rem(at - pair + pairs, pairs)).start()

        @pl.when(pair == at)
        def _():
            acc[...] = joined

    keep.wait()

    @pl.loop(1, n)
    def _(d):
        gather_arrival(d).wait_recv()

    for t in range(n):
        place = pl.ds(t * part, part)
        held = got[t].astype(jnp.float32)
        first_ref[place, :] = held[:part, :]
        second_ref[place, :] = held[slab : slab + part, :]

    @pl.loop(1, pairs)
    def _(d):
        far_copy(d).wait_recv()
        acc[...] += far[d].astype(jnp.float32)

    shared = acc[block_rows : block_rows + lines, :rank].astype(jnp.bfloat16)
    for c in range(chunks):
        fix = jnp.dot(shared, w_ref[:, pl.ds(c * cw, cw)], preferred_element_type=jnp.float32)
        for t in range(cw // 128):
            turn[pl.ds(c * (cw // 128) + t, lines, stride=tiles), :] = fix[:, t * 128 : (t + 1) * 128]
    total_ref[...] = acc[:block_rows, :] + turn[...]

    p_copy.wait_send()
    for k in range(2):
        w_copy(k).wait_send()
        forward(k).wait_send()
    for k in range(3):
        mix_copy(k).wait_send()

    @pl.loop(1, n)
    def _(d):
        spread_copy(d).wait_send()
        gather_copy(d).wait_send()

    @pl.loop(0, chips)
    def _(d):
        near_copy(d).wait_send()

    @pl.loop(0, pairs)
    def _(d):
        mid_copy(d).wait_send()

    @pl.loop(1, pairs)
    def _(d):
        far_copy(d).wait_send()


def in_hbm(array):
    return pltpu.with_memory_space_constraint(array, pltpu.HBM)


def relay(n, new_owner, old_owner, plan, x, loss, win, wout, first, second):
    micro_count, tok_rows, width = x.shape
    rows = micro_count * tok_rows
    rank = win.shape[0]
    chunks = width // column_width(width)
    block_rows = first.shape[0] // 2
    slab = -(-(block_rows // n) // 8) * 8
    lines = block_rows * 128 // width
    pad = -(-(block_rows + lines) // 16) * 16 - block_rows
    dma = pltpu.SemaphoreType.DMA
    bf16, f32 = jnp.bfloat16, jnp.float32
    group = pltpu.VMEM((n // 2, block_rows + pad, 128), bf16)
    fewer = pltpu.VMEM((n // 4, block_rows + pad, 128), bf16)
    out_lines = jax.ShapeDtypeStruct((block_rows, 128), f32)
    return pl.pallas_call(
        functools.partial(relay_kernel, n, block_rows, pad),
        out_shape=(jax.ShapeDtypeStruct((rows, width), bf16), out_lines, out_lines, out_lines),
        in_specs=[HBM] * 9,
        out_specs=(VMEM,) * 4,
        scratch_shapes=[
            pltpu.SMEM(new_owner.shape, jnp.int32),
            pltpu.SMEM(old_owner.shape, jnp.int32),
            pltpu.SMEM(plan.shape, jnp.int32),
            pltpu.SMEM((n,), jnp.int32),
            pltpu.VMEM(x.shape, bf16),
            pltpu.VMEM(x.shape, bf16),
            pltpu.VMEM(win.shape, bf16),
            pltpu.VMEM(win.shape, bf16),
            pltpu.VMEM(first.shape, f32),
            pltpu.VMEM(first.shape, f32),
            pltpu.VMEM(win.shape, bf16),
            pltpu.VMEM((rank, 128), bf16),
            pltpu.VMEM((micro_count, tok_rows, rank), bf16),
            pltpu.VMEM((micro_count, tok_rows, rank), bf16),
            pltpu.VMEM((micro_count, tok_rows, rank), bf16),
            pltpu.VMEM((n, 2, 2 * slab, 128), bf16),
            pltpu.VMEM((n, 2, 2 * slab, 128), bf16),
            pltpu.VMEM((n, 2 * slab, 128), bf16),
            pltpu.VMEM((n, 2 * slab, 128), bf16),
            pltpu.VMEM((width, rank), f32),
            pltpu.VMEM((rank, width), f32),
            pltpu.VMEM((block_rows, 128), f32),
            pltpu.VMEM((block_rows + pad, 128), f32),
            pltpu.VMEM((n, block_rows + pad, 128), bf16),
            group, group, group, fewer, fewer,
            dma((3,)), dma((4,)), dma((chunks,)), dma((chunks,)),
            dma((2,)), dma((2,)), dma((2,)), dma((2,)), dma((3,)), dma((3,)), dma, dma,
            dma((n,)), dma((n,)), dma((n,)), dma((n,)), dma((2,)),
            dma((n // 2,)), dma((n // 2,)), dma((n // 4,)), dma((n // 4,)), dma((n // 4,)), dma((n // 4,)),
        ],
        compiler_params=pltpu.CompilerParams(
            collective_id=0, has_side_effects=True, vmem_limit_bytes=44 * 1024 * 1024
        ),
        name="relay",
    )(*map(in_hbm, (new_owner, old_owner, plan, x, loss, win, wout, first, second)))


def finish_kernel(
    o_ref, total_ref, m_ref, v_ref, out_hbm, u_hbm, first_hbm, second_hbm, u_buf, first_buf, second_buf, sem
):
    count = out_hbm.shape[0]
    stores = []
    for m in range(count):
        tok_rows = out_hbm.shape[1]
        store = pltpu.make_async_copy(o_ref.at[pl.ds(m * tok_rows, tok_rows)], out_hbm.at[m], sem.at[m])
        store.start()
        stores.append(store)
    adam(total_ref[...], m_ref[...], v_ref[...], u_buf, first_buf, second_buf)
    for k, (src, dst) in enumerate(((u_buf, u_hbm), (first_buf, first_hbm), (second_buf, second_hbm))):
        store = pltpu.make_async_copy(src, dst, sem.at[count + k])
        store.start()
        stores.append(store)
    for store in stores:
        store.wait()


def finish(micro_count, o, total, m, v):
    rows, width = o.shape
    lines = jax.ShapeDtypeStruct(m.shape, jnp.float32)
    return pl.pallas_call(
        finish_kernel,
        out_shape=(
            jax.ShapeDtypeStruct((micro_count, rows // micro_count, width), jnp.bfloat16),
            lines, lines, lines,
        ),
        in_specs=[VMEM] * 4,
        out_specs=(ANY,) * 4,
        scratch_shapes=[pltpu.VMEM(m.shape, jnp.float32)] * 3 + [pltpu.SemaphoreType.DMA((micro_count + 3,))],
        compiler_params=pltpu.CompilerParams(vmem_limit_bytes=8 * 1024 * 1024),
        name="finish",
    )(o, total, m, v)


def adam(total, m, v, u_ref, first_ref, second_ref):
    grads = total / loss_scale
    first_next = beta_one * m + (1.0 - beta_one) * grads
    second_next = beta_two * v + (1.0 - beta_two) * grads * grads
    first_ref[...] = first_next
    second_ref[...] = second_next
    u_ref[...] = (
        first_next
        / (1.0 - beta_one**adam_step)
        / (jnp.sqrt(second_next / (1.0 - beta_two**adam_step)) + adam_eps)
    )


def reduce_kernel(
    n, q_ref, m_ref, v_ref, u_ref, first_ref, second_ref,
    near, summed, far, s1, r1, s2, r2,
):
    me = lax.axis_index("dp")
    core = lax.rem(me, 2)
    chip = me // 2
    chips = n // 2
    sibling = me + 1 - 2 * core
    greet(n, me, None)

    def near_copy(d):
        to = lax.rem(chip + d, chips)
        return pltpu.make_async_remote_copy(
            q_ref.at[(1 - core) * chips + to], near.at[to], s1.at[d], r1.at[d],
            device_id={"dp": sibling}, device_id_type=MESH,
        )

    def far_copy(d):
        to = lax.rem(chip + d, chips)
        return pltpu.make_async_remote_copy(
            summed.at[to], far.at[d], s2.at[d], r2.at[d],
            device_id={"dp": to * 2 + core}, device_id_type=MESH,
        )

    @pl.loop(1, chips + 1)
    def _(step):
        near_copy(lax.rem(step, chips)).start()

    @pl.loop(1, chips)
    def _(d):
        to = lax.rem(chip + d, chips)
        near_copy(d).wait_recv()
        summed[to] = (
            q_ref[core * chips + to].astype(jnp.float32) + near[to].astype(jnp.float32)
        ).astype(jnp.bfloat16)
        far_copy(d).start()

    near_copy(0).wait_recv()
    total = q_ref[core * chips + chip].astype(jnp.float32) + near[chip].astype(jnp.float32)
    first_ref[...] = total

    @pl.loop(1, chips)
    def _(d):
        far_copy(d).wait_recv()
        first_ref[...] += far[d].astype(jnp.float32)

    adam(first_ref[...], m_ref[...], v_ref[...], u_ref, first_ref, second_ref)

    @pl.loop(0, chips)
    def _(d):
        near_copy(d).wait_send()

    @pl.loop(1, chips)
    def _(d):
        far_copy(d).wait_send()


def reduce_adam(n, blocks, m, v):
    lines = m.shape
    dma = pltpu.SemaphoreType.DMA
    shape = jax.ShapeDtypeStruct(lines, jnp.float32)
    group = pltpu.VMEM((n // 2,) + lines, jnp.bfloat16)
    return pl.pallas_call(
        functools.partial(reduce_kernel, n),
        out_shape=(shape,) * 3,
        in_specs=[VMEM] * 3,
        out_specs=(VMEM,) * 3,
        scratch_shapes=[group, group, group] + [dma((n // 2,))] * 4,
        compiler_params=pltpu.CompilerParams(collective_id=1, has_side_effects=True),
        name="reduce_adam",
    )(blocks, m, v)


def passed_along(value, axis, steps):
    count = lax.axis_size(axis)
    first, last = (max(0, -steps), min(count, count - steps))
    return lax.ppermute(value, axis, [(source, source + steps) for source in range(first, last)])


def silu_slope(pre_value):
    gate_value = jax.nn.sigmoid(pre_value)
    return gate_value * (1.0 + pre_value * (1.0 - gate_value))


def per_device(
    activations,
    loss_grads,
    adapter_in,
    adapter_out,
    first_moment,
    second_moment,
    old_owner,
    new_owner,
    plan,
):
    sections = lax.axis_size("section")
    section_index = lax.axis_index("section")
    replicas = lax.axis_size("dp")
    my_index = lax.axis_index("dp")
    weight_in = adapter_in[0]
    weight_out = adapter_out[0]
    inputs_all = activations[0]
    micro_count = inputs_all.shape[0]
    tok_rows = inputs_all.shape[1]
    width = inputs_all.shape[2]
    owners_old = old_owner[0]
    owners_new = new_owner[0]
    block_len = first_moment.shape[2] // 2
    replica_ids = jnp.arange(replicas, dtype=jnp.int32)
    new_block = jnp.sum(jnp.where(owners_new == my_index, replica_ids, 0))

    def drain_turn(turn_index, state):
        previous, grad_in, grad_out, emitted = state
        received = passed_along(previous, "section", -1)
        slot = turn_index - (sections - 1 - section_index)
        is_valid = (slot >= 0) & (slot < micro_count)
        clamped = jnp.clip(slot, 0, micro_count - 1)
        micro = lax.dynamic_index_in_dim(plan, clamped, 0, keepdims=False)
        section_input = lax.dynamic_index_in_dim(inputs_all, micro, 0, keepdims=False)
        from_loss = lax.dynamic_index_in_dim(loss_grads, micro, 0, keepdims=False)
        incoming = jnp.where(section_index == sections - 1, from_loss, received)
        pre_value = jnp.dot(section_input, weight_in, preferred_element_type=jnp.float32)
        hidden = jax.nn.silu(pre_value).astype(jnp.bfloat16)
        act_grad = jnp.dot(incoming, weight_out.T, preferred_element_type=jnp.float32)
        pre_grad = (act_grad * silu_slope(pre_value)).astype(jnp.bfloat16)
        input_grad = (
            incoming.astype(jnp.float32)
            + jnp.dot(pre_grad, weight_in.T, preferred_element_type=jnp.float32)
        ).astype(jnp.bfloat16)
        valid_weight = is_valid.astype(jnp.float32)
        grad_in = grad_in + valid_weight * jnp.dot(
            section_input.T, pre_grad, preferred_element_type=jnp.float32
        )
        grad_out = grad_out + valid_weight * jnp.dot(
            hidden.T, incoming, preferred_element_type=jnp.float32
        )
        earlier = lax.dynamic_index_in_dim(emitted, clamped, 0, keepdims=False)
        written = jnp.where(is_valid, input_grad, earlier)
        emitted = lax.dynamic_update_index_in_dim(emitted, written, clamped, 0)
        return (input_grad, grad_in, grad_out, emitted)

    start_state = (
        jnp.zeros((tok_rows, width), jnp.bfloat16),
        jnp.zeros(weight_in.shape, jnp.float32),
        jnp.zeros(weight_out.shape, jnp.float32),
        jnp.zeros((micro_count, tok_rows, width), jnp.bfloat16),
    )
    place_of_block = owners_new % 2 * (replicas // 2) + owners_new // 2
    lines = (block_len // 128, 128)
    if sections == 2 and replicas % 4 == 0 and block_len % (128 * replicas) == 0:
        turned_in = weight_in.T
        row_lines = (2 * block_len // 128, 128)
        o, total, first_old, second_old = relay(
            replicas, owners_new, owners_old, plan, inputs_all, loss_grads, turned_in, weight_out,
            first_moment.reshape(row_lines), second_moment.reshape(row_lines),
        )
        emitted, update, first_next, second_next = finish(micro_count, o, total, first_old, second_old)
        shape = (1, 1, block_len)
        return (emitted[None], update.reshape(shape), first_next.reshape(shape), second_next.reshape(shape))
    last_grad, grad_in, grad_out, emitted = lax.fori_loop(
        0, micro_count + sections - 1, drain_turn, start_state
    )
    partial_value = jnp.concatenate([grad_in.reshape(-1), grad_out.reshape(-1)])
    block_at = jnp.sum(
        jnp.where(place_of_block[None, :] == replica_ids[:, None], replica_ids[None, :], 0), axis=1
    )
    blocks = jnp.take(partial_value.astype(jnp.bfloat16).reshape((replicas,) + lines), block_at, axis=0)
    old_count = owners_old.shape[0]
    piece_len = 2 * block_len // replicas
    first_pieces = first_moment[0, 0].reshape(replicas, piece_len)
    second_pieces = second_moment[0, 0].reshape(replicas, piece_len)
    first_spread = lax.all_to_all(first_pieces, "dp", split_axis=0, concat_axis=0, tiled=True)
    second_spread = lax.all_to_all(second_pieces, "dp", split_axis=0, concat_axis=0, tiled=True)
    first_held = jnp.take(first_spread, owners_old, axis=0)
    second_held = jnp.take(second_spread, owners_old, axis=0)
    my_half = my_index // old_count
    targets = owners_new.reshape(-1, 2)
    target_of_block = jnp.where(my_half == 0, targets[:, 0], targets[:, 1])
    picker = (target_of_block[None, :] == replica_ids[:, None]).astype(jnp.float32)
    first_out = jnp.dot(picker, first_held, precision=lax.Precision.HIGHEST)
    second_out = jnp.dot(picker, second_held, precision=lax.Precision.HIGHEST)
    first_got = lax.all_to_all(first_out, "dp", split_axis=0, concat_axis=0, tiled=True)
    second_got = lax.all_to_all(second_out, "dp", split_axis=0, concat_axis=0, tiled=True)
    half_start = new_block % 2 * old_count
    first_mine = lax.dynamic_slice_in_dim(first_got, half_start, old_count, 0).reshape(-1)
    second_mine = lax.dynamic_slice_in_dim(second_got, half_start, old_count, 0).reshape(-1)
    update, first_next, second_next = reduce_adam(
        replicas, blocks, first_mine.reshape(lines), second_mine.reshape(lines)
    )
    shape = (1, 1, block_len)
    return (emitted[None], update.reshape(shape), first_next.reshape(shape), second_next.reshape(shape))


def solution(mesh):
    placed = (
        P("section", None, "dp", None),
        P(None, "dp", None),
        P("section", None, None),
        P("section", None, None),
        P("section", "dp", None),
        P("section", "dp", None),
        P("section", None),
        P("section", None),
        P(),
    )
    return jax.shard_map(
        per_device,
        mesh=mesh,
        in_specs=placed,
        out_specs=(
            P("section", None, "dp", None),
            P("section", "dp", None),
            P("section", "dp", None),
            P("section", "dp", None),
        ),
        check_vma=False,
    )
```

```python
import functools
import math

import jax
import jax.numpy as jnp
from jax import lax
from jax.experimental import pallas as pl
from jax.experimental.pallas import tpu as pltpu
from jax.sharding import PartitionSpec as P

beta_one = 0.9
beta_two = 0.95
adam_eps = 1e-08
adam_step = 1000.0
loss_scale = 4096.0
MESH = pl.DeviceIdType.MESH
VMEM = pl.BlockSpec(memory_space=pltpu.VMEM)
SMEM = pl.BlockSpec(memory_space=pltpu.SMEM)
ANY = pl.BlockSpec(memory_space=pl.ANY)
HBM = pl.BlockSpec(memory_space=pltpu.HBM)


def nt_dot(left, right):
    return lax.dot_general(left, right, (((1,), (1,)), ((), ())), preferred_element_type=jnp.float32)


def column_width(width):
    return 128 * max(d for d in range(1, 8) if (width // 128) % d == 0)


def greet(n, me, extra):
    barrier = pltpu.get_barrier_semaphore()

    @pl.loop(1, n)
    def _(d):
        pl.semaphore_signal(barrier, inc=1, device_id={"dp": lax.rem(me + d, n)}, device_id_type=MESH)

    if extra is not None:
        pl.semaphore_signal(barrier, inc=1, device_id={"section": extra}, device_id_type=MESH)
    pl.semaphore_wait(barrier, n - 1 + (extra is not None))


def relay_kernel(
    n, block_rows, pad,
    new_hbm, old_hbm, plan_hbm, x_hbm, l_hbm, win_hbm, wout_hbm, m_hbm, v_hbm,
    o_ref, total_ref, first_ref, second_ref,
    new_ref, old_ref, plan_ref, order, x_buf, l_buf, win_buf, wout_buf, m_buf, v_buf, w_ref, mix_out, mix, mix_t, act_buf,
    p_out, p_got, p_up, p_now, pieces, spread, chosen, got, gin, gout, turn, acc,
    blocks, outbox, near, summed, mid, far,
    i_sem, g_sem, x_sem, l_sem, w_send, w_recv, f_send, f_recv, k_send, k_recv, j_send, j_recv, p_send, p_recv,
    a_send, a_recv, b_send, b_recv, own_sem, s1, r1, s2, r2, s3, r3,
):
    me = lax.axis_index("dp")
    section = lax.axis_index("section")
    other = 1 - section
    core = lax.rem(me, 2)
    sibling = me + 1 - 2 * core
    chip = me // 2
    chips = n // 2
    pairs = chips // 2
    lane = lax.rem(chip, 2)
    pair = chip // 2
    across = (pair * 2 + 1 - lane) * 2
    rank, width = win_hbm.shape
    cw = column_width(width)
    chunks = width // cw
    tiles = width // 128
    lines = block_rows // tiles

    barrier = pltpu.get_barrier_semaphore()

    @pl.loop(1, n)
    def _(d):
        pl.semaphore_signal(barrier, inc=1, device_id={"dp": lax.rem(me + d, n)}, device_id_type=MESH)

    for peer in (me, sibling, across + core, across + 1 - core):
        pl.semaphore_signal(barrier, inc=1, device_id={"section": other, "dp": peer}, device_id_type=MESH)

    def started(src, dst, sem):
        load = pltpu.make_async_copy(src, dst, sem)
        load.start()
        return load

    ints = [
        started(src, dst, i_sem.at[k])
        for k, (src, dst) in enumerate(((new_hbm, new_ref), (old_hbm, old_ref), (plan_hbm, plan_ref)))
    ]
    weights = [
        started(src, dst, g_sem.at[k])
        for k, (src, dst) in enumerate(
            ((m_hbm, m_buf), (v_hbm, v_buf), (win_hbm, win_buf), (wout_hbm, wout_buf))
        )
    ]
    micro_count, tok_rows, _ = x_buf.shape
    rows = micro_count * tok_rows
    edges = [micro_count * k // 8 for k in (0, 4, 6, 8)]
    spans = [pl.ds(a, b - a) for a, b in zip(edges, edges[1:])]
    loads = []
    for g, span in enumerate(spans):
        loads.append(started(x_hbm.at[span], x_buf.at[span], x_sem.at[g]))
        loads.append(started(l_hbm.at[span], l_buf.at[span], l_sem.at[g]))

    half, quarter = rank // 2, rank // 4

    def rows_of(core_at, lane_at):
        return pl.ds(pl.multiple_of(core_at * half + lane_at * quarter, quarter), quarter)

    parts = (rows_of(core, lane), rows_of(core, 1 - lane))
    their_parts = (rows_of(1 - core, lane), rows_of(1 - core, 1 - lane))

    low = pl.ds(0, tiles // 2 * 128)
    high = pl.ds(tiles // 2 * 128, width - tiles // 2 * 128)

    def lend(src, cols):
        return pltpu.make_async_remote_copy(
            src.at[parts[0], cols], w_ref.at[parts[0], low], w_send.at[0], w_recv.at[0],
            device_id={"section": other}, device_id_type=MESH,
        )

    def w_copy(k):
        spot = (parts[0], high) if k == 2 else (parts[1],)
        return pltpu.make_async_remote_copy(
            win_hbm.at[spot], w_ref.at[spot], w_send.at[k], w_recv.at[k],
            device_id={"section": other}, device_id_type=MESH,
        )

    def forward(k):
        return pltpu.make_async_remote_copy(
            w_ref.at[parts[k]], w_ref.at[parts[k]], f_send.at[k], f_recv.at[k],
            device_id={"dp": sibling}, device_id_type=MESH,
        )

    def forwarded(k):
        return pltpu.make_async_remote_copy(
            w_ref.at[their_parts[k]], w_ref.at[their_parts[k]], f_send.at[k], f_recv.at[k],
            device_id={"dp": sibling}, device_id_type=MESH,
        )

    group = (
        (me, rows_of(core, lane)),
        (sibling, rows_of(1 - core, lane)),
        (across + core, rows_of(core, 1 - lane)),
        (across + 1 - core, rows_of(1 - core, 1 - lane)),
    )

    def mix_copy(k):
        return pltpu.make_async_remote_copy(
            mix_out, mix.at[parts[0]], k_send, k_recv,
            device_id={"dp": group[k][0]}, device_id_type=MESH,
        )

    def mix_t_copy(k):
        return pltpu.make_async_remote_copy(
            mix_out, mix_t.at[parts[0]], j_send, j_recv,
            device_id={"section": other, "dp": group[k][0]}, device_id_type=MESH,
        )

    def p_copy(k):
        return pltpu.make_async_remote_copy(
            p_out.at[k], p_got.at[k], p_send.at[k], p_recv.at[k], device_id={"section": other}, device_id_type=MESH
        )

    def spread_copy(d):
        peer = lax.rem(me + d, n)
        return pltpu.make_async_remote_copy(
            pieces.at[peer], spread.at[me], a_send, a_recv,
            device_id={"dp": peer}, device_id_type=MESH,
        )

    def spread_all():
        return pltpu.make_async_remote_copy(
            pieces.at[pl.ds(0, n - 1)], spread.at[pl.ds(0, n - 1)], a_send, a_recv,
            device_id={"dp": sibling}, device_id_type=MESH,
        )

    def gather_copy(d):
        peer = lax.rem(me + d, n)
        return pltpu.make_async_remote_copy(
            chosen.at[peer], got.at[me], b_send, b_recv,
            device_id={"dp": peer}, device_id_type=MESH,
        )

    def gather_all():
        return pltpu.make_async_remote_copy(
            chosen.at[pl.ds(0, n - 1)], got.at[pl.ds(0, n - 1)], b_send, b_recv,
            device_id={"dp": sibling}, device_id_type=MESH,
        )

    def near_copy(to):
        return pltpu.make_async_remote_copy(
            outbox.at[to], near.at[to], s1, r1.at[to], device_id={"dp": sibling}, device_id_type=MESH
        )

    def mid_copy(at):
        return pltpu.make_async_remote_copy(
            summed.at[at * 2 + 1 - lane], mid.at[at], s3, r3.at[at],
            device_id={"dp": across + core}, device_id_type=MESH,
        )

    def far_copy(d):
        to = lax.rem(pair + d, pairs) * 2 + lane
        return pltpu.make_async_remote_copy(
            summed.at[to], far.at[d], s2, r2.at[d],
            device_id={"dp": to * 2 + core}, device_id_type=MESH,
        )

    pl.semaphore_wait(barrier, n + 3)

    @pl.when(section == 0)
    def _():
        lend(wout_hbm, high).start()

    @pl.when(section == 1)
    def _():
        lend(win_hbm, low).start()


    part = block_rows // n
    slab = pieces.shape[2] // 2
    filler = [jnp.zeros((slab - part, 128), jnp.float32)] if slab > part else []
    weights[0].wait()
    weights[1].wait()
    for t in range(n):
        for h in range(2):
            start = h * block_rows + t * part
            pieces[t, h] = jnp.concatenate(
                [m_buf[start : start + part, :]] + filler + [v_buf[start : start + part, :]] + filler, axis=0
            ).astype(jnp.bfloat16)

    @pl.loop(1, n)
    def _(d):
        spread_copy(d).start()

    own = started(pieces.at[me], spread.at[me], own_sem.at[0])
    for load in ints:
        load.wait()
    owners = [new_ref[c] for c in range(n)]
    for t in range(n):
        block = jnp.int32(0)
        for c in range(1, n):
            block = jnp.where(owners[c] == t, c, block)
        order[t] = block
    for b in range(n):
        blocks[b, block_rows:, :] = jnp.zeros((pad, 128), jnp.bfloat16)


    def tokens(ref, cols):
        return ref[:, :, cols].reshape(rows, -1)

    weights[2].wait()
    weights[3].wait()
    pres, acts, slopes = [], [], []
    sent = 0
    for g, span in enumerate(spans):
        loads[2 * g].wait()
        loads[2 * g + 1].wait()
        pres.append(nt_dot(x_buf[span].reshape(-1, width), win_buf[...]))
        acts.append(nt_dot(l_buf[span].reshape(-1, width), wout_buf[...]))
        slopes.append(silu_slope(pres[-1]))
        if 2 * edges[g + 1] >= (sent + 1) * micro_count:
            grad = jnp.concatenate(acts, axis=0) * jnp.concatenate(slopes, axis=0)
            top = sent * rows // 2
            p_out[sent] = jnp.concatenate(
                [grad[top : top + rows // 4], grad[top + rows // 4 : top + rows // 2]], axis=1
            ).astype(jnp.bfloat16)

            @pl.when(section == 1)
            def _():
                p_copy(sent).start()

            sent += 1
    pre, act, slope = (jnp.concatenate(parts_of, axis=0) for parts_of in (pres, acts, slopes))
    hidden_t = jax.nn.silu(pre).T.astype(jnp.bfloat16)
    act_buf[...] = act

    lend(win_hbm, low).wait_recv()

    def mixed(weight, cols):
        value = nt_dot(w_ref[parts[0], low], weight[:, cols])
        value = jnp.concatenate([value, jnp.zeros((quarter, 128 - rank), jnp.float32)], axis=1)
        return value.astype(jnp.bfloat16)

    @pl.when(section == 0)
    def _():
        mix_out[...] = mixed(wout_buf, low)
        mix[parts[0], :] = mix_out[...]
        for k in range(1, 4):
            mix_copy(k).start()

    @pl.when(section == 1)
    def _():
        mix_out[...] = mixed(win_buf, high)
        for k in range(4):
            mix_t_copy(k).start()

    for c in range(chunks):
        cols = pl.ds(c * cw, cw)
        gout[:, cols] = jnp.dot(hidden_t, tokens(l_buf, cols), preferred_element_type=jnp.float32)
    for b in range(chips):
        for t in range(tiles):
            turn[pl.ds(t, lines, stride=tiles), :] = gout[b * lines : (b + 1) * lines, t * 128 : (t + 1) * 128]
        blocks[chips + b, :block_rows, :] = turn[...].astype(jnp.bfloat16)

    @pl.when(section == 1)
    def _():
        p_up[...] = jnp.zeros_like(p_up)

    @pl.when(section == 0)
    def _():
        p_copy(0).wait_recv()
        p_copy(1).wait_recv()
        p_in = jnp.concatenate([p_got[k, :, c : c + rank] for k in range(2) for c in (0, rank)], axis=0)
        p_up[...] = p_in.reshape(p_up.shape)
        shared = jnp.dot(hidden_t, p_in, preferred_element_type=jnp.float32)
        shared = jnp.concatenate([shared, jnp.zeros((rank, 128 - rank), jnp.float32)], axis=1)
        for b in range(chips):
            blocks[chips + b, block_rows:, :] = jnp.concatenate(
                [shared[b * lines : (b + 1) * lines, :], jnp.zeros((pad - lines, 128), jnp.float32)], axis=0
            ).astype(jnp.bfloat16)
        pltpu.make_async_remote_copy(
            mix.at[pl.ds(0, 3 * quarter)], mix.at[pl.ds(0, 3 * quarter)], k_send, k_recv,
            device_id={"dp": sibling}, device_id_type=MESH,
        ).wait_recv()
        pltpu.make_async_remote_copy(
            mix_t, mix_t, j_send, j_recv, device_id={"section": other}, device_id_type=MESH
        ).wait_recv()
        act_buf[...] += jnp.dot(p_in, mix[:, :rank], preferred_element_type=jnp.float32) + nt_dot(
            p_in, mix_t[:, :rank]
        )

    w_copy(2).start()
    w_copy(1).start()
    grad = act_buf[...] * slope
    p_now[...] = grad.astype(jnp.bfloat16).reshape(p_now.shape)
    p_t = grad.T.astype(jnp.bfloat16)
    groups = math.gcd(tiles, chips)
    for g in range(groups):
        cols = pl.ds(g * (width // groups), width // groups)
        gin[cols, :] = jnp.dot(p_t, tokens(x_buf, cols), preferred_element_type=jnp.float32).T
        for b in range(g * chips // groups, (g + 1) * chips // groups):
            start = b * block_rows * 2
            even = gin[pl.ds(start, block_rows, stride=2), :]
            odd = gin[pl.ds(start + 1, block_rows, stride=2), :]
            blocks[b, :block_rows, :] = jnp.concatenate([even, odd], axis=1).astype(jnp.bfloat16)

    own.wait()

    spread_all().wait_recv()

    for t in range(n):
        block = order[t]
        chosen[t] = spread[old_ref[block // 2], lax.rem(block, 2)]

    @pl.loop(1, n)
    def _(d):
        gather_copy(d).start()

    keep = started(chosen.at[me], got.at[me], own_sem.at[1])
    table = [sorted(range(pairs), key=lambda at, p=p: (-abs(at - p), at)) for p in range(pairs)]
    turns = [sum(jnp.where(pair == p, table[p][k], 0) for p in range(pairs)) for k in range(pairs)]
    for side in (1 - lane, lane):
        for at in turns:
            to = at * 2 + side
            outbox[to] = blocks[order[to * 2 + 1 - core]]
            near_copy(to).start()

    for at in turns:
        to = at * 2 + 1 - lane
        near_copy(to).wait_recv()
        summed[to] = (
            blocks[order[to * 2 + core]].astype(jnp.float32) + near[to].astype(jnp.float32)
        ).astype(jnp.bfloat16)
        mid_copy(at).start()

    w_copy(2).wait_recv()
    forward(0).start()
    w_copy(1).wait_recv()
    forward(1).start()


    def drained(ref, cols):
        return jnp.concatenate([ref[plan_ref[m], :, cols] for m in range(micro_count)], axis=0)

    p_up_turn, p_now_turn = drained(p_up, slice(None)), drained(p_now, slice(None))
    forwarded(0).wait_recv()
    forwarded(1).wait_recv()

    def emit(c):
        cols = pl.ds(c * cw, cw)
        incoming = (
            drained(l_buf, cols).astype(jnp.float32) + jnp.dot(p_up_turn, w_ref[:, cols], preferred_element_type=jnp.float32)
        ).astype(jnp.bfloat16)
        o_ref[:, cols] = (
            incoming.astype(jnp.float32)
            + jnp.dot(p_now_turn, win_buf[:, cols], preferred_element_type=jnp.float32)
        ).astype(jnp.bfloat16)

    emitted = 0
    for step, at in enumerate(turns):
        until = -(-chunks * (step + 1) // pairs)
        for c in range(emitted, until):
            emit(c)
        emitted = until
        to = at * 2 + lane
        near_copy(to).wait_recv()
        mid_copy(at).wait_recv()
        joined = (
            blocks[order[to * 2 + core]].astype(jnp.float32)
            + near[to].astype(jnp.float32)
            + mid[at].astype(jnp.float32)
        )

        if step < pairs - 1:
            summed[to] = joined.astype(jnp.bfloat16)
            far_copy(lax.rem(at - pair + pairs, pairs)).start()
        else:
            acc[...] = joined

    keep.wait()

    gather_all().wait_recv()

    for t in range(n):
        place = pl.ds(t * part, part)
        held = got[t].astype(jnp.float32)
        first_ref[place, :] = held[:part, :]
        second_ref[place, :] = held[slab : slab + part, :]

    @pl.loop(1, pairs)
    def _(d):
        far_copy(d).wait_recv()
        acc[...] += far[d].astype(jnp.float32)

    shared = acc[block_rows : block_rows + lines, :rank].astype(jnp.bfloat16)
    for c in range(chunks):
        fix = jnp.dot(shared, w_ref[:, pl.ds(c * cw, cw)], preferred_element_type=jnp.float32)
        for t in range(cw // 128):
            turn[pl.ds(c * (cw // 128) + t, lines, stride=tiles), :] = fix[:, t * 128 : (t + 1) * 128]
    total_ref[...] = acc[:block_rows, :] + turn[...]

    lend(win_hbm, low).wait_send()
    for k in range(2):
        w_copy(k + 1).wait_send()
        forward(k).wait_send()

    @pl.when(section == 0)
    def _():
        pltpu.make_async_remote_copy(
            mix.at[pl.ds(0, 3 * quarter)], mix.at[pl.ds(0, 3 * quarter)], k_send, k_recv,
            device_id={"dp": sibling}, device_id_type=MESH,
        ).wait_send()

    @pl.when(section == 1)
    def _():
        p_copy(0).wait_send()
        p_copy(1).wait_send()
        pltpu.make_async_remote_copy(
            mix_t, mix_t, j_send, j_recv, device_id={"section": other}, device_id_type=MESH
        ).wait_send()

    spread_all().wait_send()
    gather_all().wait_send()
    pltpu.make_async_remote_copy(
        outbox, near, s1, r1.at[0], device_id={"dp": sibling}, device_id_type=MESH
    ).wait_send()
    pltpu.make_async_remote_copy(
        summed.at[pl.ds(0, pairs)], mid, s3, r3.at[0], device_id={"dp": across + core}, device_id_type=MESH
    ).wait_send()
    pltpu.make_async_remote_copy(
        summed.at[pl.ds(0, pairs - 1)], far.at[pl.ds(0, pairs - 1)], s2, r2.at[0],
        device_id={"dp": across + core}, device_id_type=MESH,
    ).wait_send()


def in_hbm(array):
    return pltpu.with_memory_space_constraint(array, pltpu.HBM)


def relay(n, new_owner, old_owner, plan, x, loss, win, wout, first, second):
    micro_count, tok_rows, width = x.shape
    rows = micro_count * tok_rows
    rank = win.shape[0]
    chunks = width // column_width(width)
    block_rows = first.shape[0] // 2
    slab = -(-(block_rows // n) // 8) * 8
    lines = block_rows * 128 // width
    pad = -(-(block_rows + lines) // 16) * 16 - block_rows
    dma = pltpu.SemaphoreType.DMA
    bf16, f32 = jnp.bfloat16, jnp.float32
    group = pltpu.VMEM((n // 2, block_rows + pad, 128), bf16)
    fewer = pltpu.VMEM((n // 4, block_rows + pad, 128), bf16)
    out_lines = jax.ShapeDtypeStruct((block_rows, 128), f32)
    return pl.pallas_call(
        functools.partial(relay_kernel, n, block_rows, pad),
        out_shape=(jax.ShapeDtypeStruct((rows, width), bf16), out_lines, out_lines, out_lines),
        in_specs=[HBM] * 9,
        out_specs=(VMEM,) * 4,
        scratch_shapes=[
            pltpu.SMEM(new_owner.shape, jnp.int32),
            pltpu.SMEM(old_owner.shape, jnp.int32),
            pltpu.SMEM(plan.shape, jnp.int32),
            pltpu.SMEM((n,), jnp.int32),
            pltpu.VMEM(x.shape, bf16),
            pltpu.VMEM(x.shape, bf16),
            pltpu.VMEM(win.shape, bf16),
            pltpu.VMEM(win.shape, bf16),
            pltpu.VMEM(first.shape, f32),
            pltpu.VMEM(first.shape, f32),
            pltpu.VMEM(win.shape, bf16),
            pltpu.VMEM((rank // 4, 128), bf16),
            pltpu.VMEM((rank, 128), bf16),
            pltpu.VMEM((rank, 128), bf16),
            pltpu.VMEM((rows, rank), f32),
            pltpu.VMEM((2, rows // 4, 2 * rank), bf16),
            pltpu.VMEM((2, rows // 4, 2 * rank), bf16),
            pltpu.VMEM((micro_count, tok_rows, rank), bf16),
            pltpu.VMEM((micro_count, tok_rows, rank), bf16),
            pltpu.VMEM((n, 2, 2 * slab, 128), bf16),
            pltpu.VMEM((n, 2, 2 * slab, 128), bf16),
            pltpu.VMEM((n, 2 * slab, 128), bf16),
            pltpu.VMEM((n, 2 * slab, 128), bf16),
            pltpu.VMEM((width, rank), f32),
            pltpu.VMEM((rank, width), f32),
            pltpu.VMEM((block_rows, 128), f32),
            pltpu.VMEM((block_rows + pad, 128), f32),
            pltpu.VMEM((n, block_rows + pad, 128), bf16),
            group, group, group, fewer, fewer,
            dma((3,)), dma((4,)), dma((3,)), dma((3,)),
            dma((3,)), dma((3,)), dma((2,)), dma((2,)), dma, dma, dma, dma, dma((2,)), dma((2,)),
            dma, dma, dma, dma, dma((2,)),
            dma, dma((n // 2,)), dma, dma((n // 4,)), dma, dma((n // 4,)),
        ],
        compiler_params=pltpu.CompilerParams(
            collective_id=0, has_side_effects=True, vmem_limit_bytes=44 * 1024 * 1024
        ),
        name="relay",
    )(*map(in_hbm, (new_owner, old_owner, plan, x, loss, win, wout, first, second)))


def finish_kernel(
    o_ref, total_ref, m_ref, v_ref, out_hbm, u_hbm, first_hbm, second_hbm, u_buf, first_buf, second_buf, sem
):
    count = out_hbm.shape[0]
    stores = []
    for m in range(count):
        tok_rows = out_hbm.shape[1]
        store = pltpu.make_async_copy(o_ref.at[pl.ds(m * tok_rows, tok_rows)], out_hbm.at[m], sem.at[m])
        store.start()
        stores.append(store)
    adam(total_ref[...], m_ref[...], v_ref[...], u_buf, first_buf, second_buf)
    for k, (src, dst) in enumerate(((u_buf, u_hbm), (first_buf, first_hbm), (second_buf, second_hbm))):
        store = pltpu.make_async_copy(src, dst, sem.at[count + k])
        store.start()
        stores.append(store)
    for store in stores:
        store.wait()


def finish(micro_count, o, total, m, v):
    rows, width = o.shape
    lines = jax.ShapeDtypeStruct(m.shape, jnp.float32)
    return pl.pallas_call(
        finish_kernel,
        out_shape=(
            jax.ShapeDtypeStruct((micro_count, rows // micro_count, width), jnp.bfloat16),
            lines, lines, lines,
        ),
        in_specs=[VMEM] * 4,
        out_specs=(ANY,) * 4,
        scratch_shapes=[pltpu.VMEM(m.shape, jnp.float32)] * 3 + [pltpu.SemaphoreType.DMA((micro_count + 3,))],
        compiler_params=pltpu.CompilerParams(vmem_limit_bytes=8 * 1024 * 1024),
        name="finish",
    )(o, total, m, v)


def adam(total, m, v, u_ref, first_ref, second_ref):
    grads = total / loss_scale
    first_next = beta_one * m + (1.0 - beta_one) * grads
    second_next = beta_two * v + (1.0 - beta_two) * grads * grads
    first_ref[...] = first_next
    second_ref[...] = second_next
    u_ref[...] = (
        first_next
        / (1.0 - beta_one**adam_step)
        / (jnp.sqrt(second_next / (1.0 - beta_two**adam_step)) + adam_eps)
    )


def reduce_kernel(
    n, q_ref, m_ref, v_ref, u_ref, first_ref, second_ref,
    near, summed, far, s1, r1, s2, r2,
):
    me = lax.axis_index("dp")
    core = lax.rem(me, 2)
    chip = me // 2
    chips = n // 2
    sibling = me + 1 - 2 * core
    greet(n, me, None)

    def near_copy(d):
        to = lax.rem(chip + d, chips)
        return pltpu.make_async_remote_copy(
            q_ref.at[(1 - core) * chips + to], near.at[to], s1.at[d], r1.at[d],
            device_id={"dp": sibling}, device_id_type=MESH,
        )

    def far_copy(d):
        to = lax.rem(chip + d, chips)
        return pltpu.make_async_remote_copy(
            summed.at[to], far.at[d], s2.at[d], r2.at[d],
            device_id={"dp": to * 2 + core}, device_id_type=MESH,
        )

    @pl.loop(1, chips + 1)
    def _(step):
        near_copy(lax.rem(step, chips)).start()

    @pl.loop(1, chips)
    def _(d):
        to = lax.rem(chip + d, chips)
        near_copy(d).wait_recv()
        summed[to] = (
            q_ref[core * chips + to].astype(jnp.float32) + near[to].astype(jnp.float32)
        ).astype(jnp.bfloat16)
        far_copy(d).start()

    near_copy(0).wait_recv()
    total = q_ref[core * chips + chip].astype(jnp.float32) + near[chip].astype(jnp.float32)
    first_ref[...] = total

    @pl.loop(1, chips)
    def _(d):
        far_copy(d).wait_recv()
        first_ref[...] += far[d].astype(jnp.float32)

    adam(first_ref[...], m_ref[...], v_ref[...], u_ref, first_ref, second_ref)

    @pl.loop(0, chips)
    def _(d):
        near_copy(d).wait_send()

    @pl.loop(1, chips)
    def _(d):
        far_copy(d).wait_send()


def reduce_adam(n, blocks, m, v):
    lines = m.shape
    dma = pltpu.SemaphoreType.DMA
    shape = jax.ShapeDtypeStruct(lines, jnp.float32)
    group = pltpu.VMEM((n // 2,) + lines, jnp.bfloat16)
    return pl.pallas_call(
        functools.partial(reduce_kernel, n),
        out_shape=(shape,) * 3,
        in_specs=[VMEM] * 3,
        out_specs=(VMEM,) * 3,
        scratch_shapes=[group, group, group] + [dma((n // 2,))] * 4,
        compiler_params=pltpu.CompilerParams(collective_id=1, has_side_effects=True),
        name="reduce_adam",
    )(blocks, m, v)


def passed_along(value, axis, steps):
    count = lax.axis_size(axis)
    first, last = (max(0, -steps), min(count, count - steps))
    return lax.ppermute(value, axis, [(source, source + steps) for source in range(first, last)])


def silu_slope(pre_value):
    gate_value = jax.nn.sigmoid(pre_value)
    return gate_value * (1.0 + pre_value * (1.0 - gate_value))


def per_device(
    activations,
    loss_grads,
    adapter_in,
    adapter_out,
    first_moment,
    second_moment,
    old_owner,
    new_owner,
    plan,
):
    sections = lax.axis_size("section")
    section_index = lax.axis_index("section")
    replicas = lax.axis_size("dp")
    my_index = lax.axis_index("dp")
    weight_in = adapter_in[0]
    weight_out = adapter_out[0]
    inputs_all = activations[0]
    micro_count = inputs_all.shape[0]
    tok_rows = inputs_all.shape[1]
    width = inputs_all.shape[2]
    owners_old = old_owner[0]
    owners_new = new_owner[0]
    block_len = first_moment.shape[2] // 2
    replica_ids = jnp.arange(replicas, dtype=jnp.int32)
    new_block = jnp.sum(jnp.where(owners_new == my_index, replica_ids, 0))

    def drain_turn(turn_index, state):
        previous, grad_in, grad_out, emitted = state
        received = passed_along(previous, "section", -1)
        slot = turn_index - (sections - 1 - section_index)
        is_valid = (slot >= 0) & (slot < micro_count)
        clamped = jnp.clip(slot, 0, micro_count - 1)
        micro = lax.dynamic_index_in_dim(plan, clamped, 0, keepdims=False)
        section_input = lax.dynamic_index_in_dim(inputs_all, micro, 0, keepdims=False)
        from_loss = lax.dynamic_index_in_dim(loss_grads, micro, 0, keepdims=False)
        incoming = jnp.where(section_index == sections - 1, from_loss, received)
        pre_value = jnp.dot(section_input, weight_in, preferred_element_type=jnp.float32)
        hidden = jax.nn.silu(pre_value).astype(jnp.bfloat16)
        act_grad = jnp.dot(incoming, weight_out.T, preferred_element_type=jnp.float32)
        pre_grad = (act_grad * silu_slope(pre_value)).astype(jnp.bfloat16)
        input_grad = (
            incoming.astype(jnp.float32)
            + jnp.dot(pre_grad, weight_in.T, preferred_element_type=jnp.float32)
        ).astype(jnp.bfloat16)
        valid_weight = is_valid.astype(jnp.float32)
        grad_in = grad_in + valid_weight * jnp.dot(
            section_input.T, pre_grad, preferred_element_type=jnp.float32
        )
        grad_out = grad_out + valid_weight * jnp.dot(
            hidden.T, incoming, preferred_element_type=jnp.float32
        )
        earlier = lax.dynamic_index_in_dim(emitted, clamped, 0, keepdims=False)
        written = jnp.where(is_valid, input_grad, earlier)
        emitted = lax.dynamic_update_index_in_dim(emitted, written, clamped, 0)
        return (input_grad, grad_in, grad_out, emitted)

    start_state = (
        jnp.zeros((tok_rows, width), jnp.bfloat16),
        jnp.zeros(weight_in.shape, jnp.float32),
        jnp.zeros(weight_out.shape, jnp.float32),
        jnp.zeros((micro_count, tok_rows, width), jnp.bfloat16),
    )
    place_of_block = owners_new % 2 * (replicas // 2) + owners_new // 2
    lines = (block_len // 128, 128)
    if sections == 2 and replicas % 4 == 0 and block_len % (128 * replicas) == 0:
        turned_in = weight_in.T
        row_lines = (2 * block_len // 128, 128)
        o, total, first_old, second_old = relay(
            replicas, owners_new, owners_old, plan, inputs_all, loss_grads, turned_in, weight_out,
            first_moment.reshape(row_lines), second_moment.reshape(row_lines),
        )
        emitted, update, first_next, second_next = finish(micro_count, o, total, first_old, second_old)
        shape = (1, 1, block_len)
        return (emitted[None], update.reshape(shape), first_next.reshape(shape), second_next.reshape(shape))
    last_grad, grad_in, grad_out, emitted = lax.fori_loop(
        0, micro_count + sections - 1, drain_turn, start_state
    )
    partial_value = jnp.concatenate([grad_in.reshape(-1), grad_out.reshape(-1)])
    block_at = jnp.sum(
        jnp.where(place_of_block[None, :] == replica_ids[:, None], replica_ids[None, :], 0), axis=1
    )
    blocks = jnp.take(partial_value.astype(jnp.bfloat16).reshape((replicas,) + lines), block_at, axis=0)
    old_count = owners_old.shape[0]
    piece_len = 2 * block_len // replicas
    first_pieces = first_moment[0, 0].reshape(replicas, piece_len)
    second_pieces = second_moment[0, 0].reshape(replicas, piece_len)
    first_spread = lax.all_to_all(first_pieces, "dp", split_axis=0, concat_axis=0, tiled=True)
    second_spread = lax.all_to_all(second_pieces, "dp", split_axis=0, concat_axis=0, tiled=True)
    first_held = jnp.take(first_spread, owners_old, axis=0)
    second_held = jnp.take(second_spread, owners_old, axis=0)
    my_half = my_index // old_count
    targets = owners_new.reshape(-1, 2)
    target_of_block = jnp.where(my_half == 0, targets[:, 0], targets[:, 1])
    picker = (target_of_block[None, :] == replica_ids[:, None]).astype(jnp.float32)
    first_out = jnp.dot(picker, first_held, precision=lax.Precision.HIGHEST)
    second_out = jnp.dot(picker, second_held, precision=lax.Precision.HIGHEST)
    first_got = lax.all_to_all(first_out, "dp", split_axis=0, concat_axis=0, tiled=True)
    second_got = lax.all_to_all(second_out, "dp", split_axis=0, concat_axis=0, tiled=True)
    half_start = new_block % 2 * old_count
    first_mine = lax.dynamic_slice_in_dim(first_got, half_start, old_count, 0).reshape(-1)
    second_mine = lax.dynamic_slice_in_dim(second_got, half_start, old_count, 0).reshape(-1)
    update, first_next, second_next = reduce_adam(
        replicas, blocks, first_mine.reshape(lines), second_mine.reshape(lines)
    )
    shape = (1, 1, block_len)
    return (emitted[None], update.reshape(shape), first_next.reshape(shape), second_next.reshape(shape))


def solution(mesh):
    placed = (
        P("section", None, "dp", None),
        P(None, "dp", None),
        P("section", None, None),
        P("section", None, None),
        P("section", "dp", None),
        P("section", "dp", None),
        P("section", None),
        P("section", None),
        P(),
    )
    return jax.shard_map(
        per_device,
        mesh=mesh,
        in_specs=placed,
        out_specs=(
            P("section", None, "dp", None),
            P("section", "dp", None),
            P("section", "dp", None),
            P("section", "dp", None),
        ),
        check_vma=False,
    )
```

```python
import functools
import math

import jax
import jax.numpy as jnp
from jax import lax
from jax.experimental import pallas as pl
from jax.experimental.pallas import tpu as pltpu
from jax.sharding import PartitionSpec as P

beta_one = 0.9
beta_two = 0.95
adam_eps = 1e-08
adam_step = 1000.0
loss_scale = 4096.0
MESH = pl.DeviceIdType.MESH
VMEM = pl.BlockSpec(memory_space=pltpu.VMEM)
SMEM = pl.BlockSpec(memory_space=pltpu.SMEM)
ANY = pl.BlockSpec(memory_space=pl.ANY)
HBM = pl.BlockSpec(memory_space=pltpu.HBM)


def nt_dot(left, right):
    return lax.dot_general(left, right, (((1,), (1,)), ((), ())), preferred_element_type=jnp.float32)


def column_width(width):
    return 128 * max(d for d in range(1, 8) if (width // 128) % d == 0)


def greet(n, me, extra):
    barrier = pltpu.get_barrier_semaphore()

    @pl.loop(1, n)
    def _(d):
        pl.semaphore_signal(barrier, inc=1, device_id={"dp": lax.rem(me + d, n)}, device_id_type=MESH)

    if extra is not None:
        pl.semaphore_signal(barrier, inc=1, device_id={"section": extra}, device_id_type=MESH)
    pl.semaphore_wait(barrier, n - 1 + (extra is not None))


def relay_kernel(
    n, block_rows, pad,
    new_hbm, old_hbm, plan_hbm, x_hbm, l_hbm, win_hbm, wout_hbm, m_hbm, v_hbm,
    o_ref, total_ref, first_ref, second_ref,
    new_ref, old_ref, plan_ref, order, x_buf, l_buf, win_buf, wout_buf, m_buf, v_buf, w_ref, mix_out, mix, mix_t, act_buf,
    p_out, p_got, p_up, p_now, pieces, spread, chosen, got, gin, gout, turn, acc,
    blocks, outbox, near, summed, mid, far,
    i_sem, g_sem, x_sem, l_sem, w_send, w_recv, f_send, f_recv, k_send, k_recv, j_send, j_recv, p_send, p_recv,
    a_send, a_recv, b_send, b_recv, own_sem, s1, r1, s2, r2, s3, r3,
):
    me = lax.axis_index("dp")
    section = lax.axis_index("section")
    other = 1 - section
    core = lax.rem(me, 2)
    sibling = me + 1 - 2 * core
    chip = me // 2
    chips = n // 2
    pairs = chips // 2
    lane = lax.rem(chip, 2)
    pair = chip // 2
    across = (pair * 2 + 1 - lane) * 2
    rank, width = win_hbm.shape
    cw = column_width(width)
    chunks = width // cw
    tiles = width // 128
    lines = block_rows // tiles

    barrier = pltpu.get_barrier_semaphore()

    @pl.loop(1, n)
    def _(d):
        pl.semaphore_signal(barrier, inc=1, device_id={"dp": lax.rem(me + d, n)}, device_id_type=MESH)

    for peer in (me, sibling, across + core, across + 1 - core):
        pl.semaphore_signal(barrier, inc=1, device_id={"section": other, "dp": peer}, device_id_type=MESH)

    def started(src, dst, sem):
        load = pltpu.make_async_copy(src, dst, sem)
        load.start()
        return load

    ints = [
        started(src, dst, i_sem.at[k])
        for k, (src, dst) in enumerate(((new_hbm, new_ref), (old_hbm, old_ref), (plan_hbm, plan_ref)))
    ]
    weights = [
        started(src, dst, g_sem.at[k])
        for k, (src, dst) in enumerate(
            ((win_hbm, win_buf), (wout_hbm, wout_buf), (m_hbm, m_buf), (v_hbm, v_buf))
        )
    ]
    micro_count, tok_rows, _ = x_buf.shape
    rows = micro_count * tok_rows
    edges = [micro_count * k // 8 for k in (0, 3, 6, 8)]
    spans = [pl.ds(a, b - a) for a, b in zip(edges, edges[1:])]
    loads = []

    def load_tokens(g):
        loads.append(started(x_hbm.at[spans[g]], x_buf.at[spans[g]], x_sem.at[g]))
        loads.append(started(l_hbm.at[spans[g]], l_buf.at[spans[g]], l_sem.at[g]))

    load_tokens(0)

    half, quarter = rank // 2, rank // 4

    def rows_of(core_at, lane_at):
        return pl.ds(pl.multiple_of(core_at * half + lane_at * quarter, quarter), quarter)

    parts = (rows_of(core, lane), rows_of(core, 1 - lane))
    their_parts = (rows_of(1 - core, lane), rows_of(1 - core, 1 - lane))

    low = pl.ds(0, tiles // 2 * 128)
    high = pl.ds(tiles // 2 * 128, width - tiles // 2 * 128)

    def lend(src, cols):
        return pltpu.make_async_remote_copy(
            src.at[parts[0], cols], w_ref.at[parts[0], low], w_send.at[0], w_recv.at[0],
            device_id={"section": other}, device_id_type=MESH,
        )

    def w_copy(k):
        spot = (parts[0], high) if k == 2 else (parts[1],)
        return pltpu.make_async_remote_copy(
            win_hbm.at[spot], w_ref.at[spot], w_send.at[k], w_recv.at[k],
            device_id={"section": other}, device_id_type=MESH,
        )

    def forward(k):
        return pltpu.make_async_remote_copy(
            w_ref.at[parts[k]], w_ref.at[parts[k]], f_send.at[k], f_recv.at[k],
            device_id={"dp": sibling}, device_id_type=MESH,
        )

    def forwarded(k):
        return pltpu.make_async_remote_copy(
            w_ref.at[their_parts[k]], w_ref.at[their_parts[k]], f_send.at[k], f_recv.at[k],
            device_id={"dp": sibling}, device_id_type=MESH,
        )

    group = (
        (me, rows_of(core, lane)),
        (sibling, rows_of(1 - core, lane)),
        (across + core, rows_of(core, 1 - lane)),
        (across + 1 - core, rows_of(1 - core, 1 - lane)),
    )

    def mix_copy(k):
        return pltpu.make_async_remote_copy(
            mix_out, mix.at[parts[0]], k_send, k_recv,
            device_id={"dp": group[k][0]}, device_id_type=MESH,
        )

    def mix_t_copy(k):
        return pltpu.make_async_remote_copy(
            mix_out, mix_t.at[parts[0]], j_send, j_recv,
            device_id={"section": other, "dp": group[k][0]}, device_id_type=MESH,
        )

    def p_copy(k):
        return pltpu.make_async_remote_copy(
            p_out.at[k], p_got.at[k], p_send.at[k], p_recv.at[k], device_id={"section": other}, device_id_type=MESH
        )

    def spread_copy(d, lane_at):
        spot = lax.rem(pair * 2 + core + d, chips)
        peer = spot // 2 * 4 + lane_at * 2 + lax.rem(spot, 2)
        return pltpu.make_async_remote_copy(
            pieces.at[peer], spread.at[me], a_send, a_recv,
            device_id={"dp": peer}, device_id_type=MESH,
        )

    def spread_all():
        return pltpu.make_async_remote_copy(
            pieces.at[pl.ds(0, n - 1)], spread.at[pl.ds(0, n - 1)], a_send, a_recv,
            device_id={"dp": sibling}, device_id_type=MESH,
        )

    def gather_copy(d):
        peer = lax.rem(me + d, n)
        return pltpu.make_async_remote_copy(
            chosen.at[peer], got.at[me], b_send, b_recv,
            device_id={"dp": peer}, device_id_type=MESH,
        )

    def gather_all():
        return pltpu.make_async_remote_copy(
            chosen.at[pl.ds(0, n - 1)], got.at[pl.ds(0, n - 1)], b_send, b_recv,
            device_id={"dp": sibling}, device_id_type=MESH,
        )

    def near_copy(to):
        return pltpu.make_async_remote_copy(
            outbox.at[to], near.at[to], s1, r1.at[to], device_id={"dp": sibling}, device_id_type=MESH
        )

    side = pair // 2
    inner = lax.rem(pair + side, 2)
    beside = pair + 1 - 2 * lax.rem(pair, 2)
    outward, inward = 3 * (1 - side), 2 - side
    turns = [
        jnp.where(inner == 1, there, here)
        for there, here in ((beside, outward), (outward, inward), (inward, beside), (pair, pair))
    ]
    cut = (block_rows + pad) // 2
    halves = (pl.ds(0, cut), pl.ds(cut, cut))

    def mid_copy(at, h):
        return pltpu.make_async_remote_copy(
            summed.at[at * 2 + 1 - lane, halves[h]], mid.at[at, halves[h]], s3, r3.at[at * 2 + h],
            device_id={"dp": across + core}, device_id_type=MESH,
        )

    def far_copy(step, h):
        at = turns[step]
        slot = jnp.where(inner == 1, 2 if step == 0 else 3, step)
        to = jnp.where(inner == 1, at, beside)
        return pltpu.make_async_remote_copy(
            summed.at[at * 2 + lane, halves[h]], far.at[slot, halves[h]], s2, r2.at[slot * 2 + h],
            device_id={"dp": (to * 2 + lane) * 2 + core}, device_id_type=MESH,
        )

    def far_arrival(slot, h):
        return pltpu.make_async_remote_copy(
            summed.at[0, halves[h]], far.at[slot, halves[h]], s2, r2.at[slot * 2 + h],
            device_id={"dp": (beside * 2 + lane) * 2 + core}, device_id_type=MESH,
        )

    part = block_rows // n
    slab = pieces.shape[2] // 2
    filler = [jnp.zeros((slab - part, 128), jnp.float32)] if slab > part else []
    weights[0].wait()
    weights[1].wait()
    load_tokens(1)
    weights[2].wait()
    weights[3].wait()
    load_tokens(2)
    for t in range(n):
        for h in range(2):
            start = h * block_rows + t * part
            pieces[t, h] = jnp.concatenate(
                [m_buf[start : start + part, :]] + filler + [v_buf[start : start + part, :]] + filler, axis=0
            ).astype(jnp.bfloat16)

    pl.semaphore_wait(barrier, n + 3)

    @pl.when(section == 0)
    def _():
        lend(wout_buf, high).start()

    @pl.when(section == 1)
    def _():
        lend(win_buf, low).start()


    @pl.loop(0, chips)
    def _(d):
        spread_copy(d, 1 - lane).start()

    @pl.loop(1, chips)
    def _(d):
        spread_copy(d, lane).start()

    own = started(pieces.at[me], spread.at[me], own_sem.at[0])
    for load in ints:
        load.wait()
    owners = [new_ref[c] for c in range(n)]
    for t in range(n):
        block = jnp.int32(0)
        for c in range(1, n):
            block = jnp.where(owners[c] == t, c, block)
        order[t] = block
    for b in range(n):
        blocks[b, block_rows:, :] = jnp.zeros((pad, 128), jnp.bfloat16)


    def tokens(ref, cols):
        return ref[:, :, cols].reshape(rows, -1)

    pres, acts, slopes = [], [], []
    sent = 0
    for g, span in enumerate(spans):
        loads[2 * g].wait()
        loads[2 * g + 1].wait()
        pres.append(nt_dot(x_buf[span].reshape(-1, width), win_buf[...]))
        acts.append(nt_dot(l_buf[span].reshape(-1, width), wout_buf[...]))
        slopes.append(silu_slope(pres[-1]))
        if 2 * edges[g + 1] >= (sent + 1) * micro_count:
            grad = jnp.concatenate(acts, axis=0) * jnp.concatenate(slopes, axis=0)
            top = sent * rows // 2
            p_out[sent] = jnp.concatenate(
                [grad[top : top + rows // 4], grad[top + rows // 4 : top + rows // 2]], axis=1
            ).astype(jnp.bfloat16)

            @pl.when(section == 1)
            def _():
                p_copy(sent).start()

            sent += 1
    pre, act, slope = (jnp.concatenate(parts_of, axis=0) for parts_of in (pres, acts, slopes))
    hidden_t = jax.nn.silu(pre).T.astype(jnp.bfloat16)
    act_buf[...] = act

    lend(win_buf, low).wait_recv()

    def mixed(weight, cols):
        value = nt_dot(w_ref[parts[0], low], weight[:, cols])
        value = jnp.concatenate([value, jnp.zeros((quarter, 128 - rank), jnp.float32)], axis=1)
        return value.astype(jnp.bfloat16)

    @pl.when(section == 0)
    def _():
        mix_out[...] = mixed(wout_buf, low)
        mix[parts[0], :] = mix_out[...]
        for k in range(1, 4):
            mix_copy(k).start()

    @pl.when(section == 1)
    def _():
        mix_out[...] = mixed(win_buf, high)
        for k in range(4):
            mix_t_copy(k).start()

    for c in range(chunks):
        cols = pl.ds(c * cw, cw)
        gout[:, cols] = jnp.dot(hidden_t, tokens(l_buf, cols), preferred_element_type=jnp.float32)
    for b in range(chips):
        for t in range(tiles):
            turn[pl.ds(t, lines, stride=tiles), :] = gout[b * lines : (b + 1) * lines, t * 128 : (t + 1) * 128]
        blocks[chips + b, :block_rows, :] = turn[...].astype(jnp.bfloat16)

    @pl.when(section == 1)
    def _():
        w_copy(2).start()
        w_copy(1).start()
        p_up[...] = jnp.zeros_like(p_up)
        blank = jnp.zeros((quarter, width), jnp.bfloat16)
        w_ref[parts[0], high] = blank[:, : width - tiles // 2 * 128]
        for spot in (parts[1], *their_parts):
            w_ref[spot, :] = blank

    @pl.when(section == 0)
    def _():
        p_copy(0).wait_recv()
        p_copy(1).wait_recv()
        p_in = jnp.concatenate([p_got[k, :, c : c + rank] for k in range(2) for c in (0, rank)], axis=0)
        p_up[...] = p_in.reshape(p_up.shape)
        shared = jnp.dot(hidden_t, p_in, preferred_element_type=jnp.float32)
        shared = jnp.concatenate([shared, jnp.zeros((rank, 128 - rank), jnp.float32)], axis=1)
        for b in range(chips):
            blocks[chips + b, block_rows:, :] = jnp.concatenate(
                [shared[b * lines : (b + 1) * lines, :], jnp.zeros((pad - lines, 128), jnp.float32)], axis=0
            ).astype(jnp.bfloat16)
        pltpu.make_async_remote_copy(
            mix.at[pl.ds(0, 3 * quarter)], mix.at[pl.ds(0, 3 * quarter)], k_send, k_recv,
            device_id={"dp": sibling}, device_id_type=MESH,
        ).wait_recv()
        pltpu.make_async_remote_copy(
            mix_t, mix_t, j_send, j_recv, device_id={"section": other}, device_id_type=MESH
        ).wait_recv()
        act_buf[...] += jnp.dot(p_in, mix[:, :rank], preferred_element_type=jnp.float32) + nt_dot(
            p_in, mix_t[:, :rank]
        )

    grad = act_buf[...] * slope
    p_now[...] = grad.astype(jnp.bfloat16).reshape(p_now.shape)
    p_t = grad.T.astype(jnp.bfloat16)
    groups = math.gcd(tiles, chips)
    for g in range(groups):
        cols = pl.ds(g * (width // groups), width // groups)
        gin[cols, :] = jnp.dot(p_t, tokens(x_buf, cols), preferred_element_type=jnp.float32).T
        for b in range(g * chips // groups, (g + 1) * chips // groups):
            start = b * block_rows * 2
            even = gin[pl.ds(start, block_rows, stride=2), :]
            odd = gin[pl.ds(start + 1, block_rows, stride=2), :]
            blocks[b, :block_rows, :] = jnp.concatenate([even, odd], axis=1).astype(jnp.bfloat16)

    for lane_at in (1 - lane, lane):
        for at in turns:
            to = at * 2 + lane_at
            outbox[to] = blocks[order[to * 2 + 1 - core]]
            near_copy(to).start()

    for at in turns:
        to = at * 2 + 1 - lane
        near_copy(to).wait_recv()
        for h, part_of in enumerate(halves):
            summed[to, part_of] = (
                blocks[order[to * 2 + core], part_of].astype(jnp.float32) + near[to, part_of].astype(jnp.float32)
            ).astype(jnp.bfloat16)
            mid_copy(at, h).start()

    own.wait()

    spread_all().wait_recv()

    for t in range(n):
        block = order[t]
        chosen[t] = spread[old_ref[block // 2], lax.rem(block, 2)]

    @pl.loop(1, n)
    def _(d):
        gather_copy(d).start()

    keep = started(chosen.at[me], got.at[me], own_sem.at[1])

    @pl.when(section == 0)
    def _():
        w_copy(2).wait_recv()
        forward(0).start()
        w_copy(1).wait_recv()
        forward(1).start()


    def drained(ref, cols):
        return jnp.concatenate([ref[plan_ref[m], :, cols] for m in range(micro_count)], axis=0)

    p_up_turn, p_now_turn = drained(p_up, slice(None)), drained(p_now, slice(None))

    def emit(c):
        cols = pl.ds(c * cw, cw)
        incoming = (
            drained(l_buf, cols).astype(jnp.float32)
            + jnp.dot(p_up_turn, w_ref[:, cols], preferred_element_type=jnp.float32)
        ).astype(jnp.bfloat16)
        o_ref[:, cols] = (
            incoming.astype(jnp.float32)
            + jnp.dot(p_now_turn, win_buf[:, cols], preferred_element_type=jnp.float32)
        ).astype(jnp.bfloat16)

    emitted = 0
    for step, at in enumerate(turns):
        to = at * 2 + lane
        near_copy(to).wait_recv()
        for h, part_of in enumerate(halves):
            mid_copy(at, h).wait_recv()
            joined = (
                blocks[order[to * 2 + core], part_of].astype(jnp.float32)
                + near[to, part_of].astype(jnp.float32)
                + mid[at, part_of].astype(jnp.float32)
            )
            if step == pairs - 1:
                acc[part_of, :] = joined
                continue
            summed[to, part_of] = joined.astype(jnp.bfloat16)
            if step > 0:

                @pl.when(inner == 1)
                def _():
                    far_arrival(step - 1, h).wait_recv()
                    summed[to, part_of] = (joined + far[step - 1, part_of].astype(jnp.float32)).astype(jnp.bfloat16)

            far_copy(step, h).start()
        if step == 0:

            @pl.when(section == 0)
            def _():
                forwarded(0).wait_recv()
                forwarded(1).wait_recv()

        until = (chunks * (step + 1) + pairs - 1) // pairs if step < pairs - 1 else chunks
        for c in range(emitted, until):
            emit(c)
        emitted = until

    keep.wait()

    gather_all().wait_recv()

    for t in range(n):
        place = pl.ds(t * part, part)
        held = got[t].astype(jnp.float32)
        first_ref[place, :] = held[:part, :]
        second_ref[place, :] = held[slab : slab + part, :]

    for slot in (2, 3):
        for h, part_of in enumerate(halves):
            far_arrival(slot, h).wait_recv()
            acc[part_of, :] += far[slot, part_of].astype(jnp.float32)

    shared = acc[block_rows : block_rows + lines, :rank].astype(jnp.bfloat16)
    for c in range(chunks):
        fix = jnp.dot(shared, w_ref[:, pl.ds(c * cw, cw)], preferred_element_type=jnp.float32)
        for t in range(cw // 128):
            turn[pl.ds(c * (cw // 128) + t, lines, stride=tiles), :] = fix[:, t * 128 : (t + 1) * 128]
    total_ref[...] = acc[:block_rows, :] + turn[...]

    lend(win_buf, low).wait_send()

    @pl.when(section == 0)
    def _():
        forward(0).wait_send()
        forward(1).wait_send()
        pltpu.make_async_remote_copy(
            mix.at[pl.ds(0, 3 * quarter)], mix.at[pl.ds(0, 3 * quarter)], k_send, k_recv,
            device_id={"dp": sibling}, device_id_type=MESH,
        ).wait_send()

    @pl.when(section == 1)
    def _():
        w_copy(1).wait_send()
        w_copy(2).wait_send()
        p_copy(0).wait_send()
        p_copy(1).wait_send()
        pltpu.make_async_remote_copy(
            mix_t, mix_t, j_send, j_recv, device_id={"section": other}, device_id_type=MESH
        ).wait_send()

    spread_all().wait_send()
    gather_all().wait_send()
    pltpu.make_async_remote_copy(
        outbox, near, s1, r1.at[0], device_id={"dp": sibling}, device_id_type=MESH
    ).wait_send()
    pltpu.make_async_remote_copy(
        summed.at[pl.ds(0, pairs)], mid, s3, r3.at[0], device_id={"dp": across + core}, device_id_type=MESH
    ).wait_send()
    pltpu.make_async_remote_copy(
        summed.at[pl.ds(0, 3)], far.at[pl.ds(0, 3)], s2, r2.at[0],
        device_id={"dp": across + core}, device_id_type=MESH,
    ).wait_send()


def in_hbm(array):
    return pltpu.with_memory_space_constraint(array, pltpu.HBM)


def relay(n, new_owner, old_owner, plan, x, loss, win, wout, first, second):
    micro_count, tok_rows, width = x.shape
    rows = micro_count * tok_rows
    rank = win.shape[0]
    chunks = width // column_width(width)
    block_rows = first.shape[0] // 2
    slab = -(-(block_rows // n) // 8) * 8
    lines = block_rows * 128 // width
    pad = -(-(block_rows + lines) // 16) * 16 - block_rows
    dma = pltpu.SemaphoreType.DMA
    bf16, f32 = jnp.bfloat16, jnp.float32
    group = pltpu.VMEM((n // 2, block_rows + pad, 128), bf16)
    fewer = pltpu.VMEM((n // 4, block_rows + pad, 128), bf16)
    out_lines = jax.ShapeDtypeStruct((block_rows, 128), f32)
    return pl.pallas_call(
        functools.partial(relay_kernel, n, block_rows, pad),
        out_shape=(jax.ShapeDtypeStruct((rows, width), bf16), out_lines, out_lines, out_lines),
        in_specs=[HBM] * 9,
        out_specs=(VMEM,) * 4,
        scratch_shapes=[
            pltpu.SMEM(new_owner.shape, jnp.int32),
            pltpu.SMEM(old_owner.shape, jnp.int32),
            pltpu.SMEM(plan.shape, jnp.int32),
            pltpu.SMEM((n,), jnp.int32),
            pltpu.VMEM(x.shape, bf16),
            pltpu.VMEM(x.shape, bf16),
            pltpu.VMEM(win.shape, bf16),
            pltpu.VMEM(win.shape, bf16),
            pltpu.VMEM(first.shape, f32),
            pltpu.VMEM(first.shape, f32),
            pltpu.VMEM(win.shape, bf16),
            pltpu.VMEM((rank // 4, 128), bf16),
            pltpu.VMEM((rank, 128), bf16),
            pltpu.VMEM((rank, 128), bf16),
            pltpu.VMEM((rows, rank), f32),
            pltpu.VMEM((2, rows // 4, 2 * rank), bf16),
            pltpu.VMEM((2, rows // 4, 2 * rank), bf16),
            pltpu.VMEM((micro_count, tok_rows, rank), bf16),
            pltpu.VMEM((micro_count, tok_rows, rank), bf16),
            pltpu.VMEM((n, 2, 2 * slab, 128), bf16),
            pltpu.VMEM((n, 2, 2 * slab, 128), bf16),
            pltpu.VMEM((n, 2 * slab, 128), bf16),
            pltpu.VMEM((n, 2 * slab, 128), bf16),
            pltpu.VMEM((width, rank), f32),
            pltpu.VMEM((rank, width), f32),
            pltpu.VMEM((block_rows, 128), f32),
            pltpu.VMEM((block_rows + pad, 128), f32),
            pltpu.VMEM((n, block_rows + pad, 128), bf16),
            group, group, group, fewer, fewer,
            dma((3,)), dma((4,)), dma((3,)), dma((3,)),
            dma((3,)), dma((3,)), dma((2,)), dma((2,)), dma, dma, dma, dma, dma((2,)), dma((2,)),
            dma, dma, dma, dma, dma((2,)),
            dma, dma((n // 2,)), dma, dma((8,)), dma, dma((n // 2,)),
        ],
        compiler_params=pltpu.CompilerParams(
            collective_id=0, has_side_effects=True, vmem_limit_bytes=44 * 1024 * 1024
        ),
        name="relay",
    )(*map(in_hbm, (new_owner, old_owner, plan, x, loss, win, wout, first, second)))


def finish_kernel(
    o_ref, total_ref, m_ref, v_ref, out_hbm, u_hbm, first_hbm, second_hbm, u_buf, first_buf, second_buf, sem
):
    count = out_hbm.shape[0]
    stores = []
    for m in range(count):
        tok_rows = out_hbm.shape[1]
        store = pltpu.make_async_copy(o_ref.at[pl.ds(m * tok_rows, tok_rows)], out_hbm.at[m], sem.at[m])
        store.start()
        stores.append(store)
    adam(total_ref[...], m_ref[...], v_ref[...], u_buf, first_buf, second_buf)
    for k, (src, dst) in enumerate(((u_buf, u_hbm), (first_buf, first_hbm), (second_buf, second_hbm))):
        store = pltpu.make_async_copy(src, dst, sem.at[count + k])
        store.start()
        stores.append(store)
    for store in stores:
        store.wait()


def finish(micro_count, o, total, m, v):
    rows, width = o.shape
    lines = jax.ShapeDtypeStruct(m.shape, jnp.float32)
    return pl.pallas_call(
        finish_kernel,
        out_shape=(
            jax.ShapeDtypeStruct((micro_count, rows // micro_count, width), jnp.bfloat16),
            lines, lines, lines,
        ),
        in_specs=[VMEM] * 4,
        out_specs=(ANY,) * 4,
        scratch_shapes=[pltpu.VMEM(m.shape, jnp.float32)] * 3 + [pltpu.SemaphoreType.DMA((micro_count + 3,))],
        compiler_params=pltpu.CompilerParams(vmem_limit_bytes=8 * 1024 * 1024),
        name="finish",
    )(o, total, m, v)


def adam(total, m, v, u_ref, first_ref, second_ref):
    grads = total / loss_scale
    first_next = beta_one * m + (1.0 - beta_one) * grads
    second_next = beta_two * v + (1.0 - beta_two) * grads * grads
    first_ref[...] = first_next
    second_ref[...] = second_next
    u_ref[...] = (
        first_next
        / (1.0 - beta_one**adam_step)
        / (jnp.sqrt(second_next / (1.0 - beta_two**adam_step)) + adam_eps)
    )


def reduce_kernel(
    n, q_ref, m_ref, v_ref, u_ref, first_ref, second_ref,
    near, summed, far, s1, r1, s2, r2,
):
    me = lax.axis_index("dp")
    core = lax.rem(me, 2)
    chip = me // 2
    chips = n // 2
    sibling = me + 1 - 2 * core
    greet(n, me, None)

    def near_copy(d):
        to = lax.rem(chip + d, chips)
        return pltpu.make_async_remote_copy(
            q_ref.at[(1 - core) * chips + to], near.at[to], s1.at[d], r1.at[d],
            device_id={"dp": sibling}, device_id_type=MESH,
        )

    def far_copy(d):
        to = lax.rem(chip + d, chips)
        return pltpu.make_async_remote_copy(
            summed.at[to], far.at[d], s2.at[d], r2.at[d],
            device_id={"dp": to * 2 + core}, device_id_type=MESH,
        )

    @pl.loop(1, chips + 1)
    def _(step):
        near_copy(lax.rem(step, chips)).start()

    @pl.loop(1, chips)
    def _(d):
        to = lax.rem(chip + d, chips)
        near_copy(d).wait_recv()
        summed[to] = (
            q_ref[core * chips + to].astype(jnp.float32) + near[to].astype(jnp.float32)
        ).astype(jnp.bfloat16)
        far_copy(d).start()

    near_copy(0).wait_recv()
    total = q_ref[core * chips + chip].astype(jnp.float32) + near[chip].astype(jnp.float32)
    first_ref[...] = total

    @pl.loop(1, chips)
    def _(d):
        far_copy(d).wait_recv()
        first_ref[...] += far[d].astype(jnp.float32)

    adam(first_ref[...], m_ref[...], v_ref[...], u_ref, first_ref, second_ref)

    @pl.loop(0, chips)
    def _(d):
        near_copy(d).wait_send()

    @pl.loop(1, chips)
    def _(d):
        far_copy(d).wait_send()


def reduce_adam(n, blocks, m, v):
    lines = m.shape
    dma = pltpu.SemaphoreType.DMA
    shape = jax.ShapeDtypeStruct(lines, jnp.float32)
    group = pltpu.VMEM((n // 2,) + lines, jnp.bfloat16)
    return pl.pallas_call(
        functools.partial(reduce_kernel, n),
        out_shape=(shape,) * 3,
        in_specs=[VMEM] * 3,
        out_specs=(VMEM,) * 3,
        scratch_shapes=[group, group, group] + [dma((n // 2,))] * 4,
        compiler_params=pltpu.CompilerParams(collective_id=1, has_side_effects=True),
        name="reduce_adam",
    )(blocks, m, v)


def passed_along(value, axis, steps):
    count = lax.axis_size(axis)
    first, last = (max(0, -steps), min(count, count - steps))
    return lax.ppermute(value, axis, [(source, source + steps) for source in range(first, last)])


def silu_slope(pre_value):
    gate_value = jax.nn.sigmoid(pre_value)
    return gate_value * (1.0 + pre_value * (1.0 - gate_value))


def per_device(
    activations,
    loss_grads,
    adapter_in,
    adapter_out,
    first_moment,
    second_moment,
    old_owner,
    new_owner,
    plan,
):
    sections = lax.axis_size("section")
    section_index = lax.axis_index("section")
    replicas = lax.axis_size("dp")
    my_index = lax.axis_index("dp")
    weight_in = adapter_in[0]
    weight_out = adapter_out[0]
    inputs_all = activations[0]
    micro_count = inputs_all.shape[0]
    tok_rows = inputs_all.shape[1]
    width = inputs_all.shape[2]
    owners_old = old_owner[0]
    owners_new = new_owner[0]
    block_len = first_moment.shape[2] // 2
    replica_ids = jnp.arange(replicas, dtype=jnp.int32)
    new_block = jnp.sum(jnp.where(owners_new == my_index, replica_ids, 0))

    def drain_turn(turn_index, state):
        previous, grad_in, grad_out, emitted = state
        received = passed_along(previous, "section", -1)
        slot = turn_index - (sections - 1 - section_index)
        is_valid = (slot >= 0) & (slot < micro_count)
        clamped = jnp.clip(slot, 0, micro_count - 1)
        micro = lax.dynamic_index_in_dim(plan, clamped, 0, keepdims=False)
        section_input = lax.dynamic_index_in_dim(inputs_all, micro, 0, keepdims=False)
        from_loss = lax.dynamic_index_in_dim(loss_grads, micro, 0, keepdims=False)
        incoming = jnp.where(section_index == sections - 1, from_loss, received)
        pre_value = jnp.dot(section_input, weight_in, preferred_element_type=jnp.float32)
        hidden = jax.nn.silu(pre_value).astype(jnp.bfloat16)
        act_grad = jnp.dot(incoming, weight_out.T, preferred_element_type=jnp.float32)
        pre_grad = (act_grad * silu_slope(pre_value)).astype(jnp.bfloat16)
        input_grad = (
            incoming.astype(jnp.float32)
            + jnp.dot(pre_grad, weight_in.T, preferred_element_type=jnp.float32)
        ).astype(jnp.bfloat16)
        valid_weight = is_valid.astype(jnp.float32)
        grad_in = grad_in + valid_weight * jnp.dot(
            section_input.T, pre_grad, preferred_element_type=jnp.float32
        )
        grad_out = grad_out + valid_weight * jnp.dot(
            hidden.T, incoming, preferred_element_type=jnp.float32
        )
        earlier = lax.dynamic_index_in_dim(emitted, clamped, 0, keepdims=False)
        written = jnp.where(is_valid, input_grad, earlier)
        emitted = lax.dynamic_update_index_in_dim(emitted, written, clamped, 0)
        return (input_grad, grad_in, grad_out, emitted)

    start_state = (
        jnp.zeros((tok_rows, width), jnp.bfloat16),
        jnp.zeros(weight_in.shape, jnp.float32),
        jnp.zeros(weight_out.shape, jnp.float32),
        jnp.zeros((micro_count, tok_rows, width), jnp.bfloat16),
    )
    place_of_block = owners_new % 2 * (replicas // 2) + owners_new // 2
    lines = (block_len // 128, 128)
    if sections == 2 and replicas == 16 and block_len % (128 * replicas) == 0:
        turned_in = weight_in.T
        row_lines = (2 * block_len // 128, 128)
        o, total, first_old, second_old = relay(
            replicas, owners_new, owners_old, plan, inputs_all, loss_grads, turned_in, weight_out,
            first_moment.reshape(row_lines), second_moment.reshape(row_lines),
        )
        emitted, update, first_next, second_next = finish(micro_count, o, total, first_old, second_old)
        shape = (1, 1, block_len)
        return (emitted[None], update.reshape(shape), first_next.reshape(shape), second_next.reshape(shape))
    last_grad, grad_in, grad_out, emitted = lax.fori_loop(
        0, micro_count + sections - 1, drain_turn, start_state
    )
    partial_value = jnp.concatenate([grad_in.reshape(-1), grad_out.reshape(-1)])
    block_at = jnp.sum(
        jnp.where(place_of_block[None, :] == replica_ids[:, None], replica_ids[None, :], 0), axis=1
    )
    blocks = jnp.take(partial_value.astype(jnp.bfloat16).reshape((replicas,) + lines), block_at, axis=0)
    old_count = owners_old.shape[0]
    piece_len = 2 * block_len // replicas
    first_pieces = first_moment[0, 0].reshape(replicas, piece_len)
    second_pieces = second_moment[0, 0].reshape(replicas, piece_len)
    first_spread = lax.all_to_all(first_pieces, "dp", split_axis=0, concat_axis=0, tiled=True)
    second_spread = lax.all_to_all(second_pieces, "dp", split_axis=0, concat_axis=0, tiled=True)
    first_held = jnp.take(first_spread, owners_old, axis=0)
    second_held = jnp.take(second_spread, owners_old, axis=0)
    my_half = my_index // old_count
    targets = owners_new.reshape(-1, 2)
    target_of_block = jnp.where(my_half == 0, targets[:, 0], targets[:, 1])
    picker = (target_of_block[None, :] == replica_ids[:, None]).astype(jnp.float32)
    first_out = jnp.dot(picker, first_held, precision=lax.Precision.HIGHEST)
    second_out = jnp.dot(picker, second_held, precision=lax.Precision.HIGHEST)
    first_got = lax.all_to_all(first_out, "dp", split_axis=0, concat_axis=0, tiled=True)
    second_got = lax.all_to_all(second_out, "dp", split_axis=0, concat_axis=0, tiled=True)
    half_start = new_block % 2 * old_count
    first_mine = lax.dynamic_slice_in_dim(first_got, half_start, old_count, 0).reshape(-1)
    second_mine = lax.dynamic_slice_in_dim(second_got, half_start, old_count, 0).reshape(-1)
    update, first_next, second_next = reduce_adam(
        replicas, blocks, first_mine.reshape(lines), second_mine.reshape(lines)
    )
    shape = (1, 1, block_len)
    return (emitted[None], update.reshape(shape), first_next.reshape(shape), second_next.reshape(shape))


def solution(mesh):
    placed = (
        P("section", None, "dp", None),
        P(None, "dp", None),
        P("section", None, None),
        P("section", None, None),
        P("section", "dp", None),
        P("section", "dp", None),
        P("section", None),
        P("section", None),
        P(),
    )
    return jax.shard_map(
        per_device,
        mesh=mesh,
        in_specs=placed,
        out_specs=(
            P("section", None, "dp", None),
            P("section", "dp", None),
            P("section", "dp", None),
            P("section", "dp", None),
        ),
        check_vma=False,
    )
```
